32 devices in a mesh: img: 8 (over z, y), sp: 4 (over x, core).
Axes of the slice: x: 2, y: 2, z: 4, core: 2. Of those that a mesh axis runs over, the one named last changes fastest.
Arguments:
- patches: bfloat16 [4096, 1280], P(('img', 'sp')), parts along dimension 0, may hold values from -6 to 6
- pos_ids: int32 [2, 4096], P(None, 'img'), parts along dimension 1, may hold values from 0 to 31, as said below
- norm_gain: float32 [1280], replicated, may hold values from 0.5 to 1.5
- norm_bias: float32 [1280], replicated, may hold values from -3 to 3
- qkv_weight: bfloat16 [1280, 3, 1280], P(None, None, 'sp')
- qkv_bias: float32 [3, 1280], replicated, may hold values from -3 to 3
- proj_weight: bfloat16 [1280, 1280], P('sp'), may hold values from -0.15625 to 0.15625
- proj_bias: float32 [1280], replicated, may hold values from -3 to 3
- merge_gain: float32 [1280], replicated, may hold values from 0.5 to 1.5
- merge_bias: float32 [1280], replicated, may hold values from -3 to 3
- fc1_weight: bfloat16 [5120, 5120], P(None, 'sp'), may hold values from -0.078125 to 0.078125
- fc1_bias: float32 [5120], P('sp'), may hold values from -3 to 3
Outputs:
- vit_out: bfloat16 [4096, 1280], P(('img', 'sp')), parts along dimension 0
- merged_hidden: bfloat16 [1024, 5120], P('img', 'sp'), parts along dimension 0
The draws below stay inside these ranges and needn't reach their ends.
There are 8 independent parts, one for each index of `img`. The reference program is written for one: setup_inputs(seed, part) draws one part's arguments, and reference() takes and returns one part's arrays. A program takes and returns all parts, laid end to end along the dimension named above; an argument that names none is the same for every part. Nothing has to cross between parts.
Inputs may be any that keep to these rules, and one draw needn't show every extreme that they name: pos_ids[0] and pos_ids[1] are the row and column of each patch on a grid of 2 R by 2 C patches, where the grid of 2x2 blocks has R rows and C columns, R C = 128, and one of R and C equals min(8, 128); each aligned run of 4 patches is one 2x2 block in row-major order inside it; every block of the grid appears once, in the order that the argument gives.
All inputs are finite; a program needn't handle non-finite values.
Results may differ from the reference program's by a relative error of at most 0.006.
Values may be sent and summed in bfloat16 or wider, within the bound.
No kernel may reach another device: no remote copies, remote signals or barrier semaphores. Data moves between devices by JAX's collectives and lax.ppermute only.
A program may use at most 64 MiB of HBM per device.

```python
import jax
import jax.numpy as jnp
from jax import lax

D = 1280
HEADS = 16
MERGE_WIDTH = 5120
PATCHES = 512
MERGED = 128


def draw_pos_ids(key, part):
    short_side = min(8, MERGED)
    long_side = MERGED // short_side
    table = jnp.array([short_side, long_side], jnp.int32)
    pick = jax.random.randint(jax.random.fold_in(key, 11), (), 0, 2)
    block_width = table[pick]
    order = jax.random.permutation(jax.random.fold_in(key, 13), MERGED).astype(jnp.int32)
    index = jnp.arange(PATCHES, dtype=jnp.int32)
    block = order[index // 4]
    inner = index % 4
    block_row = block // block_width
    block_col = block % block_width
    row = 2 * block_row + inner // 2
    col = 2 * block_col + inner % 2
    return jnp.stack([row, col]).astype(jnp.int32)


def draw_qkv_weight(key, part):
    base = jax.random.normal(key, (D, 3, D), jnp.float32) / jnp.sqrt(jnp.float32(D))
    return base.astype(jnp.bfloat16)


def block_scale(stream_key, extent, shards, smallest, top_value):
    loudness, own = 1.0, jax.random.fold_in(stream_key, 6)
    for dim, parts in shards:
        heights = jnp.exp(jax.random.uniform(jax.random.fold_in(own, dim), (parts,), jnp.float32, smallest / len(shards), top_value / len(shards)))
        loudness = loudness * jnp.repeat(heights, extent[dim] // parts).reshape([-1 if axis == dim else 1 for axis in range(len(extent))])
    return loudness


def bell_draw(stream_key, dims, spread, reach, cuts=(), held_as=jnp.bfloat16):
    values = jax.random.normal(stream_key, dims, jnp.float32) * spread
    if len(cuts) > 0:
        values = block_scale(stream_key, dims, cuts, -0.22, 0.18) * values
    return jnp.clip(values, min=-reach, max=reach).astype(held_as)


def setup_inputs(seed: int = 0, part: int = 0) -> dict:
    key_of = jax.random.split(jax.random.key(seed), 13)
    part_splits = jax.random.split(jax.random.fold_in(key_of[12], part), 13)
    patches = bell_draw(part_splits[0], (PATCHES, D), 1.0, 6.0, ((0, 4),))
    pos_ids = draw_pos_ids(jax.random.fold_in(jax.random.fold_in(key_of[12], part), 71), part)
    norm_gain = jnp.clip(1.0 + 0.1 * jax.random.normal(key_of[2], (D,), jnp.float32), 0.5, 1.5)
    norm_bias = bell_draw(key_of[3], (D,), 0.5, 3.0, (), jnp.float32)
    qkv_weight = draw_qkv_weight(jax.random.fold_in(key_of[12], 71), part)
    qkv_bias = bell_draw(key_of[5], (3, D), 0.5, 3.0, (), jnp.float32)
    proj_weight = bell_draw(key_of[6], (D, D), D ** -0.5, 0.15625, ((0, 4),))
    proj_bias = bell_draw(key_of[7], (D,), 0.5, 3.0, (), jnp.float32)
    merge_gain = jnp.clip(1.0 + 0.1 * jax.random.normal(key_of[8], (D,), jnp.float32), 0.5, 1.5)
    merge_bias = bell_draw(key_of[9], (D,), 0.5, 3.0, (), jnp.float32)
    fc1_weight = bell_draw(key_of[10], (MERGE_WIDTH, MERGE_WIDTH), MERGE_WIDTH ** -0.5, 0.078125, ((1, 4),))
    fc1_bias = bell_draw(key_of[11], (MERGE_WIDTH,), 0.5, 3.0, ((0, 4),), jnp.float32)
    return dict(patches=patches, pos_ids=pos_ids, norm_gain=norm_gain, norm_bias=norm_bias, qkv_weight=qkv_weight, qkv_bias=qkv_bias, proj_weight=proj_weight, proj_bias=proj_bias, merge_gain=merge_gain, merge_bias=merge_bias, fc1_weight=fc1_weight, fc1_bias=fc1_bias)


def layer_norm(values, gain, bias):
    mean = lax.optimization_barrier(jnp.mean(values, axis=-1, keepdims=True))
    centered = values - mean
    var = lax.optimization_barrier(jnp.mean(centered * centered, axis=-1, keepdims=True))
    return centered * lax.rsqrt(var + 1e-06) * gain + bias

def rotate(values, positions, nheads):
    count = values.shape[0]
    hdim = values.shape[1] // nheads
    quarter = hdim // 4
    inv = 1.0 / 10000.0 ** (jnp.arange(quarter, dtype=jnp.float32) * 2.0 / (hdim // 2))
    rows = positions[0].astype(jnp.float32)[:, None] * inv
    cols = positions[1].astype(jnp.float32)[:, None] * inv
    angle = jnp.concatenate([rows, cols, rows, cols], axis=1)
    cosine = jnp.cos(angle)[:, None, :]
    sine = jnp.sin(angle)[:, None, :]
    shaped = values.reshape(count, nheads, hdim)
    half = hdim // 2
    turned = jnp.concatenate([-shaped[..., half:], shaped[..., :half]], axis=-1)
    return (shaped * cosine + turned * sine).reshape(count, nheads * hdim)

def reference(patches, pos_ids, norm_gain, norm_bias, qkv_weight, qkv_bias, proj_weight, proj_bias, merge_gain, merge_bias, fc1_weight, fc1_bias):
    count = patches.shape[0]
    width = patches.shape[1]
    hdim = width // HEADS
    xfloat = patches.astype(jnp.float32)
    normed = layer_norm(xfloat, norm_gain, norm_bias).astype(jnp.bfloat16)
    qkv = jnp.dot(normed, qkv_weight.reshape(width, 3 * width), preferred_element_type=jnp.float32).reshape(count, 3, width)
    qkv = qkv + qkv_bias[None]
    query = rotate(qkv[:, 0], pos_ids, HEADS).astype(jnp.bfloat16)
    keys = rotate(qkv[:, 1], pos_ids, HEADS).astype(jnp.bfloat16)
    value = qkv[:, 2].astype(jnp.bfloat16)
    qh = query.reshape(count, HEADS, hdim).transpose(1, 0, 2)
    kh = keys.reshape(count, HEADS, hdim).transpose(1, 0, 2)
    vh = value.reshape(count, HEADS, hdim).transpose(1, 0, 2)
    scale = 1.0 / jnp.sqrt(jnp.float32(hdim))

    def one_head(triple):
        qone, kone, vone = triple
        scores = jnp.dot(qone, kone.T, preferred_element_type=jnp.float32) * scale
        top = lax.optimization_barrier(jnp.max(scores, axis=-1, keepdims=True))
        expo = jnp.exp(scores - top)
        weights = (expo / lax.optimization_barrier(jnp.sum(expo, axis=-1, keepdims=True))).astype(jnp.bfloat16)
        return jnp.dot(weights, vone, preferred_element_type=jnp.float32).astype(jnp.bfloat16)
    heads_out = lax.map(one_head, (qh, kh, vh))
    attended = heads_out.transpose(1, 0, 2).reshape(count, width)
    projected = jnp.dot(attended, proj_weight, preferred_element_type=jnp.float32)
    vit_out = (xfloat + projected + proj_bias).astype(jnp.bfloat16)
    zn = layer_norm(vit_out.astype(jnp.float32), merge_gain, merge_bias).astype(jnp.bfloat16)
    blocks = zn.reshape(count // 4, 4 * width)
    hidden = jnp.dot(blocks, fc1_weight, preferred_element_type=jnp.float32) + fc1_bias
    merged_hidden = jax.nn.gelu(hidden, approximate=False).astype(jnp.bfloat16)
    return (vit_out, merged_hidden)
```

```python
import functools
import math

import jax
import jax.numpy as jnp
from jax import lax
from jax.experimental import pallas as pl
from jax.experimental.pallas import tpu as pltpu
from jax.sharding import PartitionSpec as P

HEADS = 16
EPS = 1e-06
MIB = 1 << 20
VMEM = pl.BlockSpec(memory_space=pltpu.VMEM)
NT = (((1,), (1,)), ((), ()))
TN = (((0,), (0,)), ((), ()))
NN = (((1,), (0,)), ((), ()))


def layer_norm(values, gain, bias):
    mean = jnp.mean(values, axis=-1, keepdims=True)
    centered = values - mean
    var = jnp.mean(centered * centered, axis=-1, keepdims=True)
    return centered * lax.rsqrt(var + EPS) * gain + bias


def dot(a, b, dims):
    return lax.dot_general(a, b, dims, preferred_element_type=jnp.float32)


def call(kernel, outs, nbytes, flops, name):
    return pl.pallas_call(
        kernel,
        out_shape=outs,
        compiler_params=pltpu.CompilerParams(vmem_limit_bytes=nbytes),
        cost_estimate=pl.CostEstimate(flops=flops, bytes_accessed=1 << 20, transcendentals=0),
        name=name,
    )


def project_kernel(hdim, xa, xb, wown, wpair, gain, nbias, qbias, cosine, sine, qout, kout, vout):
    rows = xa.shape[0]
    local = wown.shape[0] // 3
    half = hdim // 2
    me = lax.axis_index("sp")
    normed = jnp.concatenate(
        [
            layer_norm(x[...].astype(jnp.float32), gain[...], nbias[...]).astype(jnp.bfloat16)
            for x in (xa, xb)
        ],
        axis=0,
    )
    cos, sin = cosine[...], sine[...]
    for side, weight in enumerate((wown, wpair)):
        owner = me if side == 0 else me ^ 1
        for c, out in enumerate((qout, kout, vout)):
            raw = dot(weight[c * local : (c + 1) * local, :], normed, NT)
            raw = raw + qbias[pl.ds(pl.multiple_of(owner * local, 8), local), c : c + 1]
            base = side * local
            if c == 2:
                out[base : base + local, :] = raw.astype(jnp.bfloat16)
                continue
            for h in range(local // hdim):
                top = raw[h * hdim : h * hdim + half]
                low = raw[h * hdim + half : (h + 1) * hdim]
                turned = jnp.concatenate([top * cos - low * sin, low * cos + top * sin], axis=0)
                out[base + h * hdim : base + (h + 1) * hdim, :] = turned.astype(jnp.bfloat16)


def attend_kernel(hdim, rows, q, kl, kr, vl, vr, pown, ppair, part, send):
    scale = math.log2(math.e) / math.sqrt(hdim)
    local = pown.shape[0]
    pieces = []
    for h in range(q.shape[0] // hdim):
        f = slice(h * hdim, (h + 1) * hdim)
        qh = q[f, 0:rows]
        sl = dot(kl[f, :], qh, TN)
        sr = dot(kr[f, :], qh, TN)
        top = jnp.maximum(jnp.max(sl, axis=0, keepdims=True), jnp.max(sr, axis=0, keepdims=True))
        el = jnp.exp2((sl - top) * scale)
        er = jnp.exp2((sr - top) * scale)
        inv = 1.0 / (jnp.sum(el, axis=0, keepdims=True) + jnp.sum(er, axis=0, keepdims=True))
        wl = (el * inv).astype(jnp.bfloat16)
        wr = (er * inv).astype(jnp.bfloat16)
        pieces.append((dot(vl[f, :], wl, NN) + dot(vr[f, :], wr, NN)).astype(jnp.bfloat16))
    per = local // hdim
    mine = jnp.concatenate(pieces[:per], axis=0)
    other = jnp.concatenate(pieces[per:], axis=0)
    total = dot(mine, pown[...], TN) + dot(other, ppair[...], TN)
    part[...] = total
    send[...] = total.astype(jnp.bfloat16)


def merge_kernel(x, part, got, pbias, gain, bias, blocks, *rest):
    scratch = rest[-1]
    width = x.shape[1]
    value = x[...].astype(jnp.float32) + (part[...] + got[...].astype(jnp.float32)) + pbias[...]
    vit = value.astype(jnp.bfloat16)
    if len(rest) == 2:
        rest[0][...] = vit
    normed = layer_norm(vit.astype(jnp.float32), gain[...], bias[...])
    count = x.shape[0] // 4
    lanes = scratch.shape[2]
    for t in range(width // lanes):
        scratch[t] = normed[:, t * lanes : (t + 1) * lanes]
        for j in range(4):
            at = j * width + t * lanes
            blocks[:, at : at + lanes] = scratch[t, pl.ds(j, count, stride=4), :].astype(jnp.bfloat16)


def gelu(v):
    return 0.5 * v * (1.0 + lax.erf(v * math.sqrt(0.5)))


def hidden_kernel(own, pair, weight, bias, *rest):
    out = rest[-1]
    me = lax.axis_index("sp")
    count = own.shape[0]
    both = jnp.concatenate([own[...], pair[...]], axis=0)
    hid = gelu(dot(both, weight[...], NN) + bias[...]).astype(jnp.bfloat16)
    if len(rest) == 1:
        start = 0
    else:
        early = rest[0]
        chip = me // 2
        out[pl.ds(pl.multiple_of(chip * 2 * count, 2 * count), 2 * count), :] = early[...]
        start = (1 - chip) * 2 * count
    core = me % 2
    out[pl.ds(pl.multiple_of(start + core * count, count), count), :] = hid[:count]
    out[pl.ds(pl.multiple_of(start + (1 - core) * count, count), count), :] = hid[count:]


def shape(dims, dtype=jnp.bfloat16):
    return jax.ShapeDtypeStruct(dims, dtype)


def two_chips(
    patches,
    pos_ids,
    norm_gain,
    norm_bias,
    qkv_weight,
    qkv_bias,
    proj_weight,
    proj_bias,
    merge_gain,
    merge_bias,
    fc1_weight,
    fc1_bias,
):
    me = lax.axis_index("sp")
    prow, width = patches.shape
    hdim = width // HEADS
    local = qkv_weight.shape[2]
    hidden = fc1_weight.shape[1]

    def swap(value, bit):
        return lax.ppermute(value, "sp", [(i, i ^ bit) for i in range(4)])

    weight = qkv_weight.transpose(1, 2, 0).reshape(3 * local, width)
    x_pair = swap(patches, 1)
    x_far = swap(patches, 2)
    w_pair = swap(weight, 1)
    p_pair = swap(proj_weight, 1)
    x_farpair = swap(x_far, 1)

    quarter = hdim // 4
    inv = 1.0 / 10000.0 ** (jnp.arange(quarter, dtype=jnp.float32) * 2.0 / (hdim // 2))

    def tables(blocks):
        pos = jnp.concatenate(
            [lax.dynamic_slice_in_dim(pos_ids, b * prow, prow, 1) for b in blocks], axis=1
        ).astype(jnp.float32)
        angle = jnp.concatenate([inv[:, None] * pos[0:1], inv[:, None] * pos[1:2]], axis=0)
        return jnp.cos(angle), jnp.sin(angle)

    row = lambda v: v.reshape(1, -1)
    qbias = qkv_bias.T
    both = 2 * local
    part_shape = (shape((prow, width), jnp.float32), shape((prow, width)))

    def project(xa, xb, blocks, name):
        cos, sin = tables(blocks)
        outs = tuple(shape((both, 2 * prow)) for _ in range(3))
        return call(
            functools.partial(project_kernel, hdim), outs, 24 * MIB, 2 * 2 * prow * width * 3 * both, name
        )(xa, xb, weight, w_pair, row(norm_gain), row(norm_bias), qbias, cos, sin)

    ql, kl, vl = project(patches, x_pair, (me, me ^ 1), "near")
    qr, kr, vr = project(x_far, x_farpair, (me ^ 2, me ^ 3), "far")

    def attend(q, name):
        return call(
            functools.partial(attend_kernel, hdim, prow), part_shape, 24 * MIB, 4 * prow * 4 * prow * both, name
        )(q, kl, kr, vl, vr, proj_weight, p_pair)

    part1, send1 = attend(qr, "attend1")
    got0 = swap(send1, 2)
    part0, send0 = attend(ql, "attend0")
    got1 = swap(send0, 2)

    def merge(x, part, got, outs, name):
        return pl.pallas_call(
            merge_kernel,
            out_shape=outs,
            scratch_shapes=[pltpu.VMEM((width // 128, prow, 128), jnp.float32)],
            compiler_params=pltpu.CompilerParams(vmem_limit_bytes=16 * MIB),
            cost_estimate=pl.CostEstimate(flops=1 << 27, bytes_accessed=1 << 20, transcendentals=0),
            name=name,
        )(x, part, got, row(proj_bias), row(merge_gain), row(merge_bias))

    bshape = shape((prow // 4, 4 * width))
    blocks0, vit = merge(patches, part0, got0, (bshape, shape((prow, width))), "merge0")
    pair0 = swap(blocks0, 1)
    fc1 = pltpu.with_memory_space_constraint(fc1_weight, pltpu.VMEM)
    flops = 2 * prow // 2 * 4 * width * hidden
    early = call(hidden_kernel, shape((prow // 2, hidden)), 24 * MIB, flops, "hidden0")(
        blocks0, pair0, fc1, row(fc1_bias)
    )
    (blocks1,) = merge(x_far, part1, got1, (bshape,), "merge1")
    pair1 = swap(blocks1, 1)
    out = call(hidden_kernel, shape((prow, hidden)), 24 * MIB, flops, "hidden1")(
        blocks1, pair1, fc1, row(fc1_bias), early
    )
    return vit, out


def rotate(values, positions, nheads):
    count = values.shape[0]
    hdim = values.shape[1] // nheads
    quarter = hdim // 4
    inv = 1.0 / 10000.0 ** (jnp.arange(quarter, dtype=jnp.float32) * 2.0 / (hdim // 2))
    rows = positions[0].astype(jnp.float32)[:, None] * inv
    cols = positions[1].astype(jnp.float32)[:, None] * inv
    angle = jnp.concatenate([rows, cols, rows, cols], axis=1)
    cosine = jnp.cos(angle)[:, None, :]
    sine = jnp.sin(angle)[:, None, :]
    shaped = values.reshape(count, nheads, hdim)
    half = hdim // 2
    turned = jnp.concatenate([-shaped[..., half:], shaped[..., :half]], axis=-1)
    return (shaped * cosine + turned * sine).reshape(count, nheads * hdim)


def attend_blocks(query, keys, value, nheads, hdim):
    count = query.shape[0]
    block = min(512, count)
    qblocks = query.reshape(count // block, block, nheads, hdim)
    kshaped = keys.reshape(count, nheads, hdim)
    vshaped = value.reshape(count, nheads, hdim)
    scale = 1.0 / jnp.sqrt(jnp.float32(hdim))

    def one_block(qpart):
        scores = jnp.einsum("bhd,khd->hbk", qpart, kshaped, preferred_element_type=jnp.float32) * scale
        top = jnp.max(scores, axis=-1, keepdims=True)
        expo = jnp.exp(scores - top)
        weights = (expo / jnp.sum(expo, axis=-1, keepdims=True)).astype(jnp.bfloat16)
        result = jnp.einsum("hbk,khd->bhd", weights, vshaped, preferred_element_type=jnp.float32)
        return result.astype(jnp.bfloat16).reshape(block, nheads * hdim)

    return lax.map(one_block, qblocks).reshape(count, nheads * hdim)


def any_size(
    patches,
    pos_ids,
    norm_gain,
    norm_bias,
    qkv_weight,
    qkv_bias,
    proj_weight,
    proj_bias,
    merge_gain,
    merge_bias,
    fc1_weight,
    fc1_bias,
):
    groups = lax.axis_size("sp")
    where = lax.axis_index("sp")
    prow, width = patches.shape
    heads_local = HEADS // groups
    hdim = width // HEADS
    local_width = width // groups
    xfloat = patches.astype(jnp.float32)
    normed = layer_norm(xfloat, norm_gain, norm_bias).astype(jnp.bfloat16)
    bias_local = lax.dynamic_slice_in_dim(qkv_bias, where * local_width, local_width, 1)
    qkv = (
        jnp.einsum(
            "pd,dcn->pcn",
            lax.all_gather(normed, "sp", axis=0, tiled=True),
            qkv_weight,
            preferred_element_type=jnp.float32,
        )
        + bias_local[None]
    )
    query = rotate(qkv[:, 0], pos_ids, heads_local).astype(jnp.bfloat16)
    keys = rotate(qkv[:, 1], pos_ids, heads_local).astype(jnp.bfloat16)
    value = qkv[:, 2].astype(jnp.bfloat16)
    attended = attend_blocks(query, keys, value, heads_local, hdim)
    returned = lax.all_to_all(attended, "sp", split_axis=0, concat_axis=1, tiled=True)
    projected = jnp.dot(
        returned,
        lax.all_gather(proj_weight, "sp", axis=0, tiled=True),
        preferred_element_type=jnp.float32,
    )
    vit_out = (xfloat + projected + proj_bias).astype(jnp.bfloat16)
    zn = layer_norm(vit_out.astype(jnp.float32), merge_gain, merge_bias).astype(jnp.bfloat16)
    blocks = zn.reshape(prow // 4, 4 * width)
    hidden = (
        jnp.dot(
            lax.all_gather(blocks, "sp", axis=0, tiled=True),
            fc1_weight,
            preferred_element_type=jnp.float32,
        )
        + fc1_bias
    )
    merged_hidden = jax.nn.gelu(hidden, approximate=False).astype(jnp.bfloat16)
    return (vit_out, merged_hidden)


def per_device(*args):
    if lax.axis_size("sp") == 4:
        return two_chips(*args)
    return any_size(*args)


def solution(mesh):
    return jax.shard_map(
        per_device,
        mesh=mesh,
        in_specs=(
            P(("img", "sp"), None),
            P(None, "img"),
            P(),
            P(),
            P(None, None, "sp"),
            P(),
            P("sp", None),
            P(),
            P(),
            P(),
            P(None, "sp"),
            P("sp"),
        ),
        out_specs=(P(("img", "sp"), None), P("img", "sp")),
        check_vma=False,
    )
```

```python
import functools
import math

import jax
import jax.numpy as jnp
from jax import lax
from jax.experimental import pallas as pl
from jax.experimental.pallas import tpu as pltpu
from jax.sharding import PartitionSpec as P


HEADS = 16
EPS = 1e-06
MIB = 1 << 20
VMEM = pl.BlockSpec(memory_space=pltpu.VMEM)
ANY = pl.BlockSpec(memory_space=pl.ANY)
NT = (((1,), (1,)), ((), ()))
TN = (((0,), (0,)), ((), ()))
NN = (((1,), (0,)), ((), ()))


def layer_norm(values, gain, bias):
    mean = jnp.mean(values, axis=-1, keepdims=True)
    centered = values - mean
    var = jnp.mean(centered * centered, axis=-1, keepdims=True)
    return centered * lax.rsqrt(var + EPS) * gain + bias


def dot(a, b, dims):
    return lax.dot_general(a, b, dims, preferred_element_type=jnp.float32)


def call(kernel, outs, nbytes, flops):
    return pl.pallas_call(
        kernel,
        out_shape=outs,
        compiler_params=pltpu.CompilerParams(vmem_limit_bytes=nbytes),
        cost_estimate=pl.CostEstimate(flops=flops, bytes_accessed=1 << 20, transcendentals=0),
    )


def norm_kernel(x, gain, bias, *rest):
    out = rest[-1]
    out[...] = layer_norm(x[...].astype(jnp.float32), gain[...], bias[...]).astype(jnp.bfloat16)


def column(qbias, owner, local, c):
    return qbias[pl.ds(pl.multiple_of(owner * local, 8), local), c : c + 1]


def rotated(raw, cos, sin, hdim):
    half = hdim // 2
    pieces = []
    for at in range(0, raw.shape[0], hdim):
        top, low = raw[at : at + half], raw[at + half : at + hdim]
        pieces += [top * cos - low * sin, low * cos + top * sin]
    return jnp.concatenate(pieces, axis=0).astype(jnp.bfloat16)


def paired(query, hdim):
    zero = jnp.zeros((hdim, query.shape[1]), query.dtype)
    rows = []
    for at in range(0, query.shape[0], 2 * hdim):
        rows.append(jnp.concatenate([query[at : at + hdim], zero], axis=1))
        rows.append(jnp.concatenate([zero, query[at + hdim : at + 2 * hdim]], axis=1))
    return jnp.concatenate(rows, axis=0)


def near_kernel(hdim, xa, xb, wown, wpair, qbias, cosine, sine, qout, kout, vout):
    local = wown.shape[0] // 3
    rows = xa.shape[0]
    me = lax.axis_index("sp")
    normed = jnp.concatenate([xa[...], xb[...]], axis=0)
    cos, sin = cosine[...], sine[...]
    for side, weight in enumerate((wown, wpair)):
        owner = me ^ side
        base = slice(side * local, (side + 1) * local)
        part = lambda c: dot(weight[c * local : (c + 1) * local, :], normed, NT) + column(qbias, owner, local, c)
        query = dot(weight[0:local, :], normed[:rows], NT) + column(qbias, owner, local, 0)
        qout[base, :] = paired(rotated(query, cos[:, :rows], sin[:, :rows], hdim), hdim)
        kout[base, :] = rotated(part(1), cos, sin, hdim)
        vout[base, :] = part(2).astype(jnp.bfloat16)


def first_kernel(hdim, q, k, v, tops, sums, outs):
    scale = math.log2(math.e) / math.sqrt(hdim)
    rows = q.shape[1] // 2
    for p in range(q.shape[0] // (2 * hdim)):
        f = slice(2 * p * hdim, 2 * (p + 1) * hdim)
        scores = dot(k[f, :], q[f, :], TN)
        top = jnp.max(scores, axis=0, keepdims=True)
        expo = jnp.exp2((scores - top) * scale)
        tops[p : p + 1, :] = top
        sums[p : p + 1, :] = jnp.sum(expo, axis=0, keepdims=True)
        total = dot(v[f, :], expo.astype(jnp.bfloat16), NN)
        outs[2 * p * hdim : (2 * p + 1) * hdim, :] = total[:hdim, :rows]
        outs[(2 * p + 1) * hdim : 2 * (p + 1) * hdim, :] = total[hdim:, rows:]


def far_kernel(hdim, xa, xb, wown, wpair, qbias, cosine, sine, q, tops, sums, outs, pown, ppair, part, send, kout, vout):
    scale = math.log2(math.e) / math.sqrt(hdim)
    local = wown.shape[0] // 3
    rows = xa.shape[0]
    me = lax.axis_index("sp")
    normed = jnp.concatenate([xa[...], xb[...]], axis=0)
    cos, sin = cosine[...], sine[...]
    total = None
    for side, weight in enumerate((wown, wpair)):
        owner = me ^ side
        base = slice(side * local, (side + 1) * local)
        key = rotated(
            dot(weight[local : 2 * local, :], normed, NT) + column(qbias, owner, local, 1), cos, sin, hdim
        )
        value = (dot(weight[2 * local :, :], normed, NT) + column(qbias, owner, local, 2)).astype(jnp.bfloat16)
        kout[base, :] = key
        vout[base, :] = value
        pieces = []
        for at in range(0, local, 2 * hdim):
            f = slice(side * local + at, side * local + at + 2 * hdim)
            p = (side * local + at) // (2 * hdim)
            scores = dot(key[at : at + 2 * hdim], q[f, :], TN)
            old = tops[p : p + 1, :]
            top = jnp.maximum(old, jnp.max(scores, axis=0, keepdims=True))
            expo = jnp.exp2((scores - top) * scale)
            shrink = jnp.exp2((old - top) * scale)
            inv = 1.0 / (sums[p : p + 1, :] * shrink + jnp.sum(expo, axis=0, keepdims=True))
            late = dot(value[at : at + 2 * hdim], expo.astype(jnp.bfloat16), NN)
            for h in range(2):
                lanes = slice(h * rows, (h + 1) * rows)
                feats = slice(h * hdim, (h + 1) * hdim)
                early = outs[f.start + h * hdim : f.start + (h + 1) * hdim, :]
                mixed = (early * shrink[:, lanes] + late[feats, lanes]) * inv[:, lanes]
                pieces.append(mixed.astype(jnp.bfloat16))
        add = dot(jnp.concatenate(pieces, axis=0), (pown, ppair)[side][...], TN)
        total = add if total is None else total + add
    part[...] = total
    send[...] = total.astype(jnp.bfloat16)


def late_kernel(hdim, x, wown, wpair, qbias, cosine, sine, kn, vn, kf, vf, pown, ppair, part, send):
    scale = math.log2(math.e) / math.sqrt(hdim)
    local = wown.shape[0] // 3
    rows = x.shape[0]
    me = lax.axis_index("sp")
    total = None
    for side, weight in enumerate((wown, wpair)):
        query = dot(weight[:local, :], x[...], NT) + column(qbias, me ^ side, local, 0)
        query = paired(rotated(query, cosine[:, :rows], sine[:, :rows], hdim), hdim)
        pieces = []
        for at in range(0, local, 2 * hdim):
            f = slice(side * local + at, side * local + at + 2 * hdim)
            both = query[at : at + 2 * hdim]
            sn = dot(kn[f, :], both, TN)
            sf = dot(kf[f, :], both, TN)
            top = jnp.maximum(jnp.max(sn, axis=0, keepdims=True), jnp.max(sf, axis=0, keepdims=True))
            en = jnp.exp2((sn - top) * scale)
            ef = jnp.exp2((sf - top) * scale)
            inv = 1.0 / (jnp.sum(en, axis=0, keepdims=True) + jnp.sum(ef, axis=0, keepdims=True))
            mixed = dot(vn[f, :], (en * inv).astype(jnp.bfloat16), NN)
            mixed = (mixed + dot(vf[f, :], (ef * inv).astype(jnp.bfloat16), NN)).astype(jnp.bfloat16)
            pieces += [mixed[:hdim, :rows], mixed[hdim:, rows:]]
        add = dot(jnp.concatenate(pieces, axis=0), (pown, ppair)[side][...], TN)
        total = add if total is None else total + add
    part[...] = total
    send[...] = total.astype(jnp.bfloat16)


def merge_kernel(keep, x, part, got, pbias, gain, bias, *rest):
    blocks, scratch = rest[-2 - keep], rest[-1]
    width = x.shape[1]
    value = x[...].astype(jnp.float32) + (part[...] + got[...].astype(jnp.float32)) + pbias[...]
    vit = value.astype(jnp.bfloat16)
    if keep:
        rest[-2][...] = vit
    normed = layer_norm(vit.astype(jnp.float32), gain[...], bias[...])
    count = x.shape[0] // 4
    lanes = scratch.shape[2]
    for t in range(width // lanes):
        scratch[t] = normed[:, t * lanes : (t + 1) * lanes]
        for j in range(4):
            at = j * width + t * lanes
            blocks[:, at : at + lanes] = scratch[t, pl.ds(j, count, stride=4), :].astype(jnp.bfloat16)


def gelu(v):
    return 0.5 * v * (1.0 + lax.erf(v * math.sqrt(0.5)))


def hidden_kernel(own, pair, weight, bias, *rest):
    out = rest[-1]
    me = lax.axis_index("sp")
    count = own.shape[0]
    both = jnp.concatenate([own[...], pair[...]], axis=0)
    hid = gelu(dot(both, weight[...], NN) + bias[...]).astype(jnp.bfloat16)
    if len(rest) == 1:
        start = 0
    else:
        early = rest[0]
        chip = me // 2
        out[pl.ds(pl.multiple_of((1 - chip) * 2 * count, 2 * count), 2 * count), :] = early[...]
        start = chip * 2 * count
    core = me % 2
    out[pl.ds(pl.multiple_of(start + core * count, count), count), :] = hid[:count]
    out[pl.ds(pl.multiple_of(start + (1 - core) * count, count), count), :] = hid[count:]


def shape(dims, dtype=jnp.bfloat16):
    return jax.ShapeDtypeStruct(dims, dtype)


def two_chips(
    patches,
    pos_ids,
    norm_gain,
    norm_bias,
    qkv_weight,
    qkv_bias,
    proj_weight,
    proj_bias,
    merge_gain,
    merge_bias,
    fc1_weight,
    fc1_bias,
):
    me = lax.axis_index("sp")
    prow, width = patches.shape
    hdim = width // HEADS
    local = qkv_weight.shape[2]
    hidden = fc1_weight.shape[1]

    def swap(value, bit):
        return lax.ppermute(value, "sp", [(i, i ^ bit) for i in range(4)])

    weight = qkv_weight.transpose(1, 2, 0).reshape(3 * local, width)
    x_far = swap(patches, 2)
    x_pair = swap(patches, 1)
    w_pair = swap(weight, 1)
    p_pair = swap(proj_weight, 1)

    quarter = hdim // 4
    inv = 1.0 / 10000.0 ** (jnp.arange(quarter, dtype=jnp.float32) * 2.0 / (hdim // 2))
    pos = jnp.concatenate(
        [lax.dynamic_slice_in_dim(pos_ids, (me ^ k) * prow, prow, 1) for k in range(4)], axis=1
    ).astype(jnp.float32)
    angle = jnp.concatenate([inv[:, None] * pos[0:1], inv[:, None] * pos[1:2]], axis=0)
    cos, sin = jnp.cos(angle), jnp.sin(angle)
    cos_near, cos_far = cos[:, : 2 * prow], cos[:, 2 * prow :]
    sin_near, sin_far = sin[:, : 2 * prow], sin[:, 2 * prow :]

    row = lambda v: v.reshape(1, -1)
    qbias = qkv_bias.T
    both = 2 * local
    tall = shape((both, 2 * prow))
    part_shape = (shape((prow, width), jnp.float32), shape((prow, width)))
    mul = 2 * prow * width * local * 2
    gain, nbias = row(norm_gain), row(norm_bias)

    def norm(x, *after):
        return pl.pallas_call(
            norm_kernel,
            out_shape=shape((prow, width)),
            in_specs=[VMEM] * 3 + [ANY] * len(after),
            compiler_params=pltpu.CompilerParams(vmem_limit_bytes=8 * MIB),
            cost_estimate=pl.CostEstimate(flops=mul // 4, bytes_accessed=1 << 20, transcendentals=0),
        )(x, gain, nbias, *after)

    n_own = norm(patches)
    n_pair = norm(x_pair)
    q_near, k_near, v_near = call(
        functools.partial(near_kernel, hdim), (tall, tall, tall), 24 * MIB, 6 * mul
    )(n_own, n_pair, weight, w_pair, qbias, cos_near, sin_near)
    state = tuple(shape((HEADS // 4, 2 * prow), jnp.float32) for _ in range(2))
    tops, sums, outs = call(
        functools.partial(first_kernel, hdim), state + (shape((both, prow), jnp.float32),), 24 * MIB, 2 * mul
    )(q_near, k_near, v_near)

    n_far = norm(x_far, tops)
    n_farpair = swap(n_far, 1)
    part0, send0, k_far, v_far = call(
        functools.partial(far_kernel, hdim), part_shape + (tall, tall), 24 * MIB, 6 * mul
    )(n_far, n_farpair, weight, w_pair, qbias, cos_far, sin_far, q_near, tops, sums, outs, proj_weight, p_pair)
    got1 = swap(send0, 2)
    part1, send1 = call(
        functools.partial(late_kernel, hdim), part_shape, 24 * MIB, 6 * mul
    )(n_far, weight, w_pair, qbias, cos_far, sin_far, k_near, v_near, k_far, v_far, proj_weight, p_pair)
    got0 = swap(send1, 2)

    pbias = row(proj_bias)

    def merge(keep, x, part, got, outs, *after):
        return pl.pallas_call(
            functools.partial(merge_kernel, keep),
            out_shape=outs,
            in_specs=[VMEM] * 6 + [ANY] * len(after),
            scratch_shapes=[pltpu.VMEM((width // 128, prow, 128), jnp.float32)],
            compiler_params=pltpu.CompilerParams(vmem_limit_bytes=16 * MIB),
            cost_estimate=pl.CostEstimate(flops=mul // 4, bytes_accessed=1 << 20, transcendentals=0),
        )(x, part, got, pbias, row(merge_gain), row(merge_bias), *after)

    bshape = shape((prow // 4, 4 * width))
    (blocks1,) = merge(0, x_far, part1, got1, (bshape,))
    pair1 = swap(blocks1, 1)
    fc1 = pltpu.with_memory_space_constraint(fc1_weight, pltpu.VMEM)
    flops = 2 * prow // 2 * 4 * width * hidden
    early = call(hidden_kernel, shape((prow // 2, hidden)), 24 * MIB, flops)(blocks1, pair1, fc1, row(fc1_bias))
    blocks0, vit = merge(1, patches, part0, got0, (bshape, shape((prow, width))), early)
    pair0 = swap(blocks0, 1)
    out = call(hidden_kernel, shape((prow, hidden)), 24 * MIB, flops)(blocks0, pair0, fc1, row(fc1_bias), early)
    return vit, out


def rotate(values, positions, nheads):
    count = values.shape[0]
    hdim = values.shape[1] // nheads
    quarter = hdim // 4
    inv = 1.0 / 10000.0 ** (jnp.arange(quarter, dtype=jnp.float32) * 2.0 / (hdim // 2))
    rows = positions[0].astype(jnp.float32)[:, None] * inv
    cols = positions[1].astype(jnp.float32)[:, None] * inv
    angle = jnp.concatenate([rows, cols, rows, cols], axis=1)
    cosine = jnp.cos(angle)[:, None, :]
    sine = jnp.sin(angle)[:, None, :]
    shaped = values.reshape(count, nheads, hdim)
    half = hdim // 2
    turned = jnp.concatenate([-shaped[..., half:], shaped[..., :half]], axis=-1)
    return (shaped * cosine + turned * sine).reshape(count, nheads * hdim)


def attend_blocks(query, keys, value, nheads, hdim):
    count = query.shape[0]
    block = min(512, count)
    qblocks = query.reshape(count // block, block, nheads, hdim)
    kshaped = keys.reshape(count, nheads, hdim)
    vshaped = value.reshape(count, nheads, hdim)
    scale = 1.0 / jnp.sqrt(jnp.float32(hdim))

    def one_block(qpart):
        scores = jnp.einsum("bhd,khd->hbk", qpart, kshaped, preferred_element_type=jnp.float32) * scale
        top = jnp.max(scores, axis=-1, keepdims=True)
        expo = jnp.exp(scores - top)
        weights = (expo / jnp.sum(expo, axis=-1, keepdims=True)).astype(jnp.bfloat16)
        result = jnp.einsum("hbk,khd->bhd", weights, vshaped, preferred_element_type=jnp.float32)
        return result.astype(jnp.bfloat16).reshape(block, nheads * hdim)

    return lax.map(one_block, qblocks).reshape(count, nheads * hdim)


def any_size(
    patches,
    pos_ids,
    norm_gain,
    norm_bias,
    qkv_weight,
    qkv_bias,
    proj_weight,
    proj_bias,
    merge_gain,
    merge_bias,
    fc1_weight,
    fc1_bias,
):
    groups = lax.axis_size("sp")
    where = lax.axis_index("sp")
    prow, width = patches.shape
    heads_local = HEADS // groups
    hdim = width // HEADS
    local_width = width // groups
    xfloat = patches.astype(jnp.float32)
    normed = layer_norm(xfloat, norm_gain, norm_bias).astype(jnp.bfloat16)
    bias_local = lax.dynamic_slice_in_dim(qkv_bias, where * local_width, local_width, 1)
    qkv = (
        jnp.einsum(
            "pd,dcn->pcn",
            lax.all_gather(normed, "sp", axis=0, tiled=True),
            qkv_weight,
            preferred_element_type=jnp.float32,
        )
        + bias_local[None]
    )
    query = rotate(qkv[:, 0], pos_ids, heads_local).astype(jnp.bfloat16)
    keys = rotate(qkv[:, 1], pos_ids, heads_local).astype(jnp.bfloat16)
    value = qkv[:, 2].astype(jnp.bfloat16)
    attended = attend_blocks(query, keys, value, heads_local, hdim)
    returned = lax.all_to_all(attended, "sp", split_axis=0, concat_axis=1, tiled=True)
    projected = jnp.dot(
        returned,
        lax.all_gather(proj_weight, "sp", axis=0, tiled=True),
        preferred_element_type=jnp.float32,
    )
    vit_out = (xfloat + projected + proj_bias).astype(jnp.bfloat16)
    zn = layer_norm(vit_out.astype(jnp.float32), merge_gain, merge_bias).astype(jnp.bfloat16)
    blocks = zn.reshape(prow // 4, 4 * width)
    hidden = (
        jnp.dot(
            lax.all_gather(blocks, "sp", axis=0, tiled=True),
            fc1_weight,
            preferred_element_type=jnp.float32,
        )
        + fc1_bias
    )
    merged_hidden = jax.nn.gelu(hidden, approximate=False).astype(jnp.bfloat16)
    return (vit_out, merged_hidden)


def per_device(*args):
    if lax.axis_size("sp") == 4:
        return two_chips(*args)
    return any_size(*args)


def solution(mesh):
    return jax.shard_map(
        per_device,
        mesh=mesh,
        in_specs=(
            P(("img", "sp"), None),
            P(None, "img"),
            P(),
            P(),
            P(None, None, "sp"),
            P(),
            P("sp", None),
            P(),
            P(),
            P(),
            P(None, "sp"),
            P("sp"),
        ),
        out_specs=(P(("img", "sp"), None), P("img", "sp")),
        check_vma=False,
    )
```

```python
import functools
import math

import jax
import jax.numpy as jnp
from jax import lax
from jax.experimental import pallas as pl
from jax.experimental.pallas import tpu as pltpu
from jax.sharding import PartitionSpec as P


HEADS = 16
EPS = 1e-06
MIB = 1 << 20
VMEM = pl.BlockSpec(memory_space=pltpu.VMEM)
ANY = pl.BlockSpec(memory_space=pl.ANY)
NT = (((1,), (1,)), ((), ()))
TN = (((0,), (0,)), ((), ()))
NN = (((1,), (0,)), ((), ()))


def layer_norm(values, gain, bias):
    mean = jnp.mean(values, axis=-1, keepdims=True)
    centered = values - mean
    var = jnp.mean(centered * centered, axis=-1, keepdims=True)
    return centered * lax.rsqrt(var + EPS) * gain + bias


def dot(a, b, dims):
    return lax.dot_general(a, b, dims, preferred_element_type=jnp.float32)


def call(kernel, outs, nbytes, flops):
    return pl.pallas_call(
        kernel,
        out_shape=outs,
        compiler_params=pltpu.CompilerParams(vmem_limit_bytes=nbytes),
        cost_estimate=pl.CostEstimate(flops=flops, bytes_accessed=1 << 20, transcendentals=0),
    )


def setup_kernel(hdim, x, pos, qkv_bias, *rest):
    vectors, (normed, rows, qcol, cosine, sine) = rest[:-5], rest[-5:]
    width = x.shape[1]
    prow = x.shape[0]
    me = lax.axis_index("sp")
    rows[...] = jnp.zeros_like(rows)
    for at, vector in enumerate(vectors):
        rows[at : at + 1, :] = vector[...].reshape(1, width)
    cube = jnp.concatenate([qkv_bias[...], jnp.zeros((5, width), jnp.float32)], axis=0)
    qcol[...] = cube.T
    quarter = hdim // 4
    feature = lax.broadcasted_iota(jnp.int32, (2 * quarter, prow), 0)
    second = feature >= quarter
    power = jnp.where(second, feature - quarter, feature).astype(jnp.float32)
    inv = jnp.exp(power * (-2.0 * math.log(10000.0) / (hdim // 2)))
    for k in range(4):
        at = pl.ds(pl.multiple_of((me ^ k) * prow, prow), prow)
        place = jnp.where(second, pos[1:2, at], pos[0:1, at]).astype(jnp.float32)
        angle = place * inv
        cosine[:, k * prow : (k + 1) * prow] = jnp.cos(angle)
        sine[:, k * prow : (k + 1) * prow] = jnp.sin(angle)
    value = layer_norm(x[...].astype(jnp.float32), rows[0:1, :], rows[1:2, :])
    normed[...] = value.astype(jnp.bfloat16)


def copy_kernel(x, out):
    out[...] = x[...]


def norm_kernel(x, rows, *rest):
    out = rest[-1]
    out[...] = layer_norm(x[...].astype(jnp.float32), rows[0:1, :], rows[1:2, :]).astype(jnp.bfloat16)


def column(qcol, owner, local, c):
    return qcol[pl.ds(pl.multiple_of(owner * local, 8), local), c : c + 1]


def rotated(raw, cos, sin, hdim):
    half = hdim // 2
    pieces = []
    for at in range(0, raw.shape[0], hdim):
        top, low = raw[at : at + half], raw[at + half : at + hdim]
        pieces += [top * cos - low * sin, low * cos + top * sin]
    return jnp.concatenate(pieces, axis=0).astype(jnp.bfloat16)


def paired(query, hdim):
    zero = jnp.zeros((hdim, query.shape[1]), query.dtype)
    rows = []
    for at in range(0, query.shape[0], 2 * hdim):
        rows.append(jnp.concatenate([query[at : at + hdim], zero], axis=1))
        rows.append(jnp.concatenate([zero, query[at + hdim : at + 2 * hdim]], axis=1))
    return jnp.concatenate(rows, axis=0)


def near_kernel(hdim, xa, xb, wown, wfrom, pfrom, qcol, cosine, sine, qout, kout, vout, wpair, ppair, sems):
    local = wown.shape[0] // 3
    rows = xa.shape[0]
    me = lax.axis_index("sp")
    wcopy = pltpu.make_async_copy(wfrom, wpair, sems.at[0])
    pcopy = pltpu.make_async_copy(pfrom, ppair, sems.at[1])
    wcopy.start()
    pcopy.start()
    normed = jnp.concatenate([xa[...], xb[...]], axis=0)
    cos, sin = cosine[:, : 2 * rows], sine[:, : 2 * rows]
    for side, weight in enumerate((wown, wpair)):
        if side == 1:
            wcopy.wait()
        owner = me ^ side
        base = slice(side * local, (side + 1) * local)
        query = dot(weight[0:local, :], normed[:rows], NT) + column(qcol, owner, local, 0)
        qout[base, :] = paired(rotated(query, cos[:, :rows], sin[:, :rows], hdim), hdim)
        keyval = dot(weight[local:, :], normed, NT)
        kout[base, :] = rotated(keyval[:local] + column(qcol, owner, local, 1), cos, sin, hdim)
        vout[base, :] = (keyval[local:] + column(qcol, owner, local, 2)).astype(jnp.bfloat16)
    pcopy.wait()


def first_kernel(hdim, q, k, v, tops, sums, outs):
    scale = math.log2(math.e) / math.sqrt(hdim)
    rows = q.shape[1] // 2
    for p in range(q.shape[0] // (2 * hdim)):
        f = slice(2 * p * hdim, 2 * (p + 1) * hdim)
        scores = dot(k[f, :], q[f, :], TN)
        top = jnp.max(scores, axis=0, keepdims=True)
        expo = jnp.exp2((scores - top) * scale)
        tops[p : p + 1, :] = top
        sums[p : p + 1, :] = jnp.sum(expo, axis=0, keepdims=True)
        total = dot(v[f, :], expo.astype(jnp.bfloat16), NN)
        outs[2 * p * hdim : (2 * p + 1) * hdim, :] = total[:hdim, :rows]
        outs[(2 * p + 1) * hdim : 2 * (p + 1) * hdim, :] = total[hdim:, rows:]


def far_kernel(hdim, xa, xb, wown, wpair, qcol, cosine, sine, q, tops, sums, outs, pown, ppair, part, send, kout, vout):
    scale = math.log2(math.e) / math.sqrt(hdim)
    local = wown.shape[0] // 3
    rows = xa.shape[0]
    me = lax.axis_index("sp")
    normed = jnp.concatenate([xa[...], xb[...]], axis=0)
    cos, sin = cosine[:, 2 * rows :], sine[:, 2 * rows :]
    total = None
    for side, weight in enumerate((wown, wpair)):
        owner = me ^ side
        base = slice(side * local, (side + 1) * local)
        keyval = dot(weight[local:, :], normed, NT)
        key = rotated(keyval[:local] + column(qcol, owner, local, 1), cos, sin, hdim)
        value = (keyval[local:] + column(qcol, owner, local, 2)).astype(jnp.bfloat16)
        kout[base, :] = key
        vout[base, :] = value
        pieces = []
        for at in range(0, local, 2 * hdim):
            f = slice(side * local + at, side * local + at + 2 * hdim)
            p = (side * local + at) // (2 * hdim)
            scores = dot(key[at : at + 2 * hdim], q[f, :], TN)
            old = tops[p : p + 1, :]
            top = jnp.maximum(old, jnp.max(scores, axis=0, keepdims=True))
            expo = jnp.exp2((scores - top) * scale)
            shrink = jnp.exp2((old - top) * scale)
            inv = 1.0 / (sums[p : p + 1, :] * shrink + jnp.sum(expo, axis=0, keepdims=True))
            late = dot(value[at : at + 2 * hdim], expo.astype(jnp.bfloat16), NN)
            for h in range(2):
                lanes = slice(h * rows, (h + 1) * rows)
                feats = slice(h * hdim, (h + 1) * hdim)
                early = outs[f.start + h * hdim : f.start + (h + 1) * hdim, :]
                mixed = (early * shrink[:, lanes] + late[feats, lanes]) * inv[:, lanes]
                pieces.append(mixed.astype(jnp.bfloat16))
        add = dot(jnp.concatenate(pieces, axis=0), (pown, ppair)[side][...], TN)
        total = add if total is None else total + add
    part[...] = total
    send[...] = total.astype(jnp.bfloat16)


def late_kernel(hdim, x, wown, wpair, qcol, cosine, sine, kn, vn, kf, vf, pown, ppair, part, send):
    scale = math.log2(math.e) / math.sqrt(hdim)
    local = wown.shape[0] // 3
    rows = x.shape[0]
    me = lax.axis_index("sp")
    total = None
    for side, weight in enumerate((wown, wpair)):
        query = dot(weight[:local, :], x[...], NT) + column(qcol, me ^ side, local, 0)
        far = slice(2 * rows, 3 * rows)
        query = paired(rotated(query, cosine[:, far], sine[:, far], hdim), hdim)
        pieces = []
        for at in range(0, local, 2 * hdim):
            f = slice(side * local + at, side * local + at + 2 * hdim)
            both = query[at : at + 2 * hdim]
            sn = dot(kn[f, :], both, TN)
            sf = dot(kf[f, :], both, TN)
            top = jnp.maximum(jnp.max(sn, axis=0, keepdims=True), jnp.max(sf, axis=0, keepdims=True))
            en = jnp.exp2((sn - top) * scale)
            ef = jnp.exp2((sf - top) * scale)
            inv = 1.0 / (jnp.sum(en, axis=0, keepdims=True) + jnp.sum(ef, axis=0, keepdims=True))
            mixed = dot(vn[f, :], (en * inv).astype(jnp.bfloat16), NN)
            mixed = (mixed + dot(vf[f, :], (ef * inv).astype(jnp.bfloat16), NN)).astype(jnp.bfloat16)
            pieces += [mixed[:hdim, :rows], mixed[hdim:, rows:]]
        add = dot(jnp.concatenate(pieces, axis=0), (pown, ppair)[side][...], TN)
        total = add if total is None else total + add
    part[...] = total
    send[...] = total.astype(jnp.bfloat16)


def merge_kernel(x, part, got, rows, *rest):
    blocks, vit, scratch = rest[-3:]
    width = x.shape[1]
    value = x[...].astype(jnp.float32) + (part[...] + got[...].astype(jnp.float32)) + rows[2:3, :]
    rounded = value.astype(jnp.bfloat16)
    vit[...] = rounded
    normed = layer_norm(rounded.astype(jnp.float32), rows[3:4, :], rows[4:5, :])
    count = x.shape[0] // 4
    lanes = scratch.shape[2]
    for t in range(width // lanes):
        scratch[t] = normed[:, t * lanes : (t + 1) * lanes]
        for j in range(4):
            at = j * width + t * lanes
            blocks[:, at : at + lanes] = scratch[t, pl.ds(j, count, stride=4), :].astype(jnp.bfloat16)


def gelu(v):
    return 0.5 * v * (1.0 + lax.erf(v * math.sqrt(0.5)))


def hidden_kernel(last, own, pair, weight, rows, *rest):
    me = lax.axis_index("sp")
    chip, core = me // 2, me % 2
    count = own.shape[0]
    if last:
        vit, _, out, vout, stage, sems = rest
        start = chip * 2 * count
        vcopy = pltpu.make_async_copy(vit, vout, sems.at[2 * stage.shape[0]])
        vcopy.start()
    else:
        out, stage, sems = rest
        start = (1 - chip) * 2 * count
    both = jnp.concatenate([own[...], pair[...]], axis=0)
    step = stage.shape[2]
    copies = []
    for n in range(stage.shape[0]):
        cols = slice(n * step, (n + 1) * step)
        hid = gelu(dot(both, weight[:, cols], NN) + rows[5:6, cols]).astype(jnp.bfloat16)
        stage[n] = hid
        for half, place in enumerate((core, 1 - core)):
            at = pl.ds(pl.multiple_of(start + place * count, count), count)
            copy = pltpu.make_async_copy(
                stage.at[n, pl.ds(half * count, count)], out.at[at, pl.ds(n * step, step)], sems.at[2 * n + half]
            )
            copy.start()
            copies.append(copy)
    for copy in copies:
        copy.wait()
    if last:
        vcopy.wait()


def shape(dims, dtype=jnp.bfloat16):
    return jax.ShapeDtypeStruct(dims, dtype)


def two_chips(
    patches,
    pos_ids,
    norm_gain,
    norm_bias,
    qkv_weight,
    qkv_bias,
    proj_weight,
    proj_bias,
    merge_gain,
    merge_bias,
    fc1_weight,
    fc1_bias,
):
    prow, width = patches.shape
    hdim = width // HEADS
    local = qkv_weight.shape[2]
    hidden = fc1_weight.shape[1]

    def swap(value, bit):
        return lax.ppermute(value, "sp", [(i, i ^ bit) for i in range(4)])

    weight = qkv_weight.transpose(1, 2, 0).reshape(3 * local, width)
    x_far = swap(patches, 2)
    x_pair = swap(patches, 1)
    w_pair = swap(weight, 1)
    p_pair = swap(proj_weight, 1)

    both = 2 * local
    tall = shape((both, 2 * prow))
    part_shape = (shape((prow, width), jnp.float32), shape((prow, width)))
    mul = 2 * prow * width * local * 2
    table = shape((hdim // 2, 4 * prow), jnp.float32)

    n_own, rows, qcol, cos, sin = call(
        functools.partial(setup_kernel, hdim),
        (shape((prow, width)), shape((8, width), jnp.float32), shape((width, 8), jnp.float32), table, table),
        8 * MIB,
        mul,
    )(patches, pos_ids, qkv_bias, norm_gain, norm_bias, proj_bias, merge_gain, merge_bias, fc1_bias)

    def norm(x, *after):
        return pl.pallas_call(
            norm_kernel,
            out_shape=shape((prow, width)),
            in_specs=[VMEM] * 2 + [ANY] * len(after),
            compiler_params=pltpu.CompilerParams(vmem_limit_bytes=8 * MIB),
            cost_estimate=pl.CostEstimate(flops=mul // 4, bytes_accessed=1 << 20, transcendentals=0),
        )(x, rows, *after)

    n_pair = norm(x_pair)
    q_near, k_near, v_near, w_vmem, p_vmem = pl.pallas_call(
        functools.partial(near_kernel, hdim),
        out_shape=(tall, tall, tall, pltpu.VMEM(weight.shape, weight.dtype), pltpu.VMEM(proj_weight.shape, weight.dtype)),
        in_specs=[VMEM] * 3 + [ANY] * 2 + [VMEM] * 3,
        out_specs=[VMEM] * 5,
        scratch_shapes=[pltpu.SemaphoreType.DMA((2,))],
        compiler_params=pltpu.CompilerParams(vmem_limit_bytes=16 * MIB),
        cost_estimate=pl.CostEstimate(flops=6 * mul, bytes_accessed=1 << 23, transcendentals=0),
        name="near",
    )(n_own, n_pair, weight, w_pair, p_pair, qcol, cos, sin)
    state = tuple(shape((HEADS // 4, 2 * prow), jnp.float32) for _ in range(2))
    tops, sums, outs = call(
        functools.partial(first_kernel, hdim), state + (shape((both, prow), jnp.float32),), 16 * MIB, 2 * mul
    )(q_near, k_near, v_near)

    n_far = norm(x_far, tops)
    n_farpair = swap(n_far, 1)
    part0, send0, k_far, v_far = call(
        functools.partial(far_kernel, hdim), part_shape + (tall, tall), 16 * MIB, 6 * mul
    )(n_far, n_farpair, weight, w_vmem, qcol, cos, sin, q_near, tops, sums, outs, proj_weight, p_vmem)
    got1 = swap(send0, 2)
    part1, send1 = call(
        functools.partial(late_kernel, hdim), part_shape, 16 * MIB, 6 * mul
    )(n_far, weight, w_vmem, qcol, cos, sin, k_near, v_near, k_far, v_far, proj_weight, p_vmem)
    got0 = swap(send1, 2)

    late_rows = call(copy_kernel, shape(rows.shape, rows.dtype), MIB, 1000)(rows)

    def merge(x, part, got, *after):
        return pl.pallas_call(
            merge_kernel,
            out_shape=(shape((prow // 4, 4 * width)), shape((prow, width))),
            in_specs=[VMEM] * 4 + [ANY] * len(after),
            scratch_shapes=[pltpu.VMEM((width // 128, prow, 128), jnp.float32)],
            compiler_params=pltpu.CompilerParams(vmem_limit_bytes=8 * MIB),
            cost_estimate=pl.CostEstimate(flops=mul // 4, bytes_accessed=1 << 20, transcendentals=0),
        )(x, part, got, late_rows, *after)

    fc1 = pltpu.with_memory_space_constraint(fc1_weight, pltpu.VMEM)
    out_shape = shape((prow, hidden))

    def finish(blocks, pair, *more):
        last = len(more) > 0
        outs = (out_shape, shape((prow, width))) if last else (out_shape,)
        return pl.pallas_call(
            functools.partial(hidden_kernel, last),
            out_shape=outs,
            in_specs=[VMEM] * 4 + [VMEM, ANY][: len(more)],
            out_specs=[ANY] * len(outs),
            scratch_shapes=[
                pltpu.VMEM((hidden // 256, prow // 2, 256), jnp.bfloat16),
                pltpu.SemaphoreType.DMA((2 * (hidden // 256) + 1,)),
            ],
            input_output_aliases={5: 0} if last else {},
            compiler_params=pltpu.CompilerParams(vmem_limit_bytes=8 * MIB),
            cost_estimate=pl.CostEstimate(
                flops=prow * 4 * width * hidden, bytes_accessed=1 << 24, transcendentals=0
            ),
        )(blocks, pair, fc1, rows, *more)

    blocks1, _ = merge(x_far, part1, got1)
    pair1 = swap(blocks1, 1)
    (early,) = finish(blocks1, pair1)
    blocks0, vit = merge(patches, part0, got0, early)
    pair0 = swap(blocks0, 1)
    merged, vit_out = finish(blocks0, pair0, vit, early)
    return vit_out, merged


def rotate(values, positions, nheads):
    count = values.shape[0]
    hdim = values.shape[1] // nheads
    quarter = hdim // 4
    inv = 1.0 / 10000.0 ** (jnp.arange(quarter, dtype=jnp.float32) * 2.0 / (hdim // 2))
    rows = positions[0].astype(jnp.float32)[:, None] * inv
    cols = positions[1].astype(jnp.float32)[:, None] * inv
    angle = jnp.concatenate([rows, cols, rows, cols], axis=1)
    cosine = jnp.cos(angle)[:, None, :]
    sine = jnp.sin(angle)[:, None, :]
    shaped = values.reshape(count, nheads, hdim)
    half = hdim // 2
    turned = jnp.concatenate([-shaped[..., half:], shaped[..., :half]], axis=-1)
    return (shaped * cosine + turned * sine).reshape(count, nheads * hdim)


def attend_blocks(query, keys, value, nheads, hdim):
    count = query.shape[0]
    block = min(512, count)
    qblocks = query.reshape(count // block, block, nheads, hdim)
    kshaped = keys.reshape(count, nheads, hdim)
    vshaped = value.reshape(count, nheads, hdim)
    scale = 1.0 / jnp.sqrt(jnp.float32(hdim))

    def one_block(qpart):
        scores = jnp.einsum("bhd,khd->hbk", qpart, kshaped, preferred_element_type=jnp.float32) * scale
        top = jnp.max(scores, axis=-1, keepdims=True)
        expo = jnp.exp(scores - top)
        weights = (expo / jnp.sum(expo, axis=-1, keepdims=True)).astype(jnp.bfloat16)
        result = jnp.einsum("hbk,khd->bhd", weights, vshaped, preferred_element_type=jnp.float32)
        return result.astype(jnp.bfloat16).reshape(block, nheads * hdim)

    return lax.map(one_block, qblocks).reshape(count, nheads * hdim)


def any_size(
    patches,
    pos_ids,
    norm_gain,
    norm_bias,
    qkv_weight,
    qkv_bias,
    proj_weight,
    proj_bias,
    merge_gain,
    merge_bias,
    fc1_weight,
    fc1_bias,
):
    groups = lax.axis_size("sp")
    where = lax.axis_index("sp")
    prow, width = patches.shape
    heads_local = HEADS // groups
    hdim = width // HEADS
    local_width = width // groups
    xfloat = patches.astype(jnp.float32)
    normed = layer_norm(xfloat, norm_gain, norm_bias).astype(jnp.bfloat16)
    bias_local = lax.dynamic_slice_in_dim(qkv_bias, where * local_width, local_width, 1)
    qkv = (
        jnp.einsum(
            "pd,dcn->pcn",
            lax.all_gather(normed, "sp", axis=0, tiled=True),
            qkv_weight,
            preferred_element_type=jnp.float32,
        )
        + bias_local[None]
    )
    query = rotate(qkv[:, 0], pos_ids, heads_local).astype(jnp.bfloat16)
    keys = rotate(qkv[:, 1], pos_ids, heads_local).astype(jnp.bfloat16)
    value = qkv[:, 2].astype(jnp.bfloat16)
    attended = attend_blocks(query, keys, value, heads_local, hdim)
    returned = lax.all_to_all(attended, "sp", split_axis=0, concat_axis=1, tiled=True)
    projected = jnp.dot(
        returned,
        lax.all_gather(proj_weight, "sp", axis=0, tiled=True),
        preferred_element_type=jnp.float32,
    )
    vit_out = (xfloat + projected + proj_bias).astype(jnp.bfloat16)
    zn = layer_norm(vit_out.astype(jnp.float32), merge_gain, merge_bias).astype(jnp.bfloat16)
    blocks = zn.reshape(prow // 4, 4 * width)
    hidden = (
        jnp.dot(
            lax.all_gather(blocks, "sp", axis=0, tiled=True),
            fc1_weight,
            preferred_element_type=jnp.float32,
        )
        + fc1_bias
    )
    merged_hidden = jax.nn.gelu(hidden, approximate=False).astype(jnp.bfloat16)
    return (vit_out, merged_hidden)


def per_device(*args):
    if lax.axis_size("sp") == 4:
        return two_chips(*args)
    return any_size(*args)


def solution(mesh):
    return jax.shard_map(
        per_device,
        mesh=mesh,
        in_specs=(
            P(("img", "sp"), None),
            P(None, "img"),
            P(),
            P(),
            P(None, None, "sp"),
            P(),
            P("sp", None),
            P(),
            P(),
            P(),
            P(None, "sp"),
            P("sp"),
        ),
        out_specs=(P(("img", "sp"), None), P("img", "sp")),
        check_vma=False,
    )
```

```python
import functools
import math

import jax
import jax.numpy as jnp
from jax import lax
from jax.experimental import pallas as pl
from jax.experimental.pallas import tpu as pltpu
from jax.sharding import PartitionSpec as P


HEADS = 16
EPS = 1e-06
MIB = 1 << 20
VMEM = pl.BlockSpec(memory_space=pltpu.VMEM)
ANY = pl.BlockSpec(memory_space=pl.ANY)
HBM = pl.BlockSpec(memory_space=pltpu.HBM)
NT = (((1,), (1,)), ((), ()))
TN = (((0,), (0,)), ((), ()))
NN = (((1,), (0,)), ((), ()))


def layer_norm(values, gain, bias):
    mean = jnp.mean(values, axis=-1, keepdims=True)
    centered = values - mean
    var = jnp.mean(centered * centered, axis=-1, keepdims=True)
    return centered * lax.rsqrt(var + EPS) * gain + bias


def dot(a, b, dims):
    return lax.dot_general(a, b, dims, preferred_element_type=jnp.float32)


def call(kernel, outs, nbytes, flops):
    return pl.pallas_call(
        kernel,
        out_shape=outs,
        compiler_params=pltpu.CompilerParams(vmem_limit_bytes=nbytes),
        cost_estimate=pl.CostEstimate(flops=flops, bytes_accessed=1 << 20, transcendentals=0),
    )


def setup_kernel(hdim, count, *refs):
    sources, rest = refs[:count], refs[count:]
    x, wown, pown, normed, rows, qcol, cosine, sine, pos, qkv_bias = rest[:10]
    vectors, sems = rest[10:-1], rest[-1]
    targets = (x, pos, qkv_bias) + tuple(vectors) + (pown, wown)
    copies = [pltpu.make_async_copy(a, b, sems.at[n]) for n, (a, b) in enumerate(zip(sources, targets))]
    for copy in copies:
        copy.start()
    prow, width = x.shape
    me = lax.axis_index("sp")
    quarter = hdim // 4
    feature = lax.broadcasted_iota(jnp.int32, (2 * quarter, prow), 0)
    second = feature >= quarter
    power = jnp.where(second, feature - quarter, feature).astype(jnp.float32)
    inv = jnp.exp(power * (-2.0 * math.log(10000.0) / (hdim // 2)))
    rows[...] = jnp.zeros_like(rows)
    for copy in copies[:-2]:
        copy.wait()
    for k in range(4):
        at = pl.ds(pl.multiple_of((me ^ k) * prow, prow), prow)
        place = jnp.where(second, pos[1:2, at], pos[0:1, at]).astype(jnp.float32)
        angle = place * inv
        cosine[:, k * prow : (k + 1) * prow] = jnp.cos(angle)
        sine[:, k * prow : (k + 1) * prow] = jnp.sin(angle)
    for at, vector in enumerate(vectors):
        rows[at : at + 1, :] = vector[...].reshape(1, width)
    cube = jnp.concatenate([qkv_bias[...], jnp.zeros((5, width), jnp.float32)], axis=0)
    qcol[...] = cube.T
    value = layer_norm(x[...].astype(jnp.float32), rows[0:1, :], rows[1:2, :])
    normed[...] = value.astype(jnp.bfloat16)
    for copy in copies[-2:]:
        copy.wait()


def copy_kernel(x, out):
    out[...] = x[...]


def norm_kernel(x, rows, *rest):
    out = rest[-1]
    out[...] = layer_norm(x[...].astype(jnp.float32), rows[0:1, :], rows[1:2, :]).astype(jnp.bfloat16)


def column(qcol, owner, local, c):
    return qcol[pl.ds(pl.multiple_of(owner * local, 8), local), c : c + 1]


def rotated(raw, cos, sin, hdim):
    half = hdim // 2
    pieces = []
    for at in range(0, raw.shape[0], hdim):
        top, low = raw[at : at + half], raw[at + half : at + hdim]
        pieces += [top * cos - low * sin, low * cos + top * sin]
    return jnp.concatenate(pieces, axis=0).astype(jnp.bfloat16)


def paired(query, hdim):
    zero = jnp.zeros((hdim, query.shape[1]), query.dtype)
    rows = []
    for at in range(0, query.shape[0], 2 * hdim):
        rows.append(jnp.concatenate([query[at : at + hdim], zero], axis=1))
        rows.append(jnp.concatenate([zero, query[at + hdim : at + 2 * hdim]], axis=1))
    return jnp.concatenate(rows, axis=0)


def near_kernel(hdim, side, xa, xb, weight, qcol, cosine, sine, qout, kout, vout, tops, sums, outs):
    scale = math.log2(math.e) / math.sqrt(hdim)
    local = weight.shape[0] // 3
    rows = xa.shape[0]
    owner = lax.axis_index("sp") ^ side
    normed = jnp.concatenate([xa[...], xb[...]], axis=0)
    cos, sin = cosine[:, : 2 * rows], sine[:, : 2 * rows]
    query = dot(weight[0:local, :], normed[:rows], NT) + column(qcol, owner, local, 0)
    query = paired(rotated(query, cos[:, :rows], sin[:, :rows], hdim), hdim)
    keyval = dot(weight[local:, :], normed, NT)
    key = rotated(keyval[:local] + column(qcol, owner, local, 1), cos, sin, hdim)
    value = (keyval[local:] + column(qcol, owner, local, 2)).astype(jnp.bfloat16)
    qout[...] = query
    kout[...] = key
    vout[...] = value
    for p in range(local // (2 * hdim)):
        f = slice(2 * p * hdim, 2 * (p + 1) * hdim)
        scores = dot(key[f], query[f], TN)
        top = jnp.max(scores, axis=0, keepdims=True)
        expo = jnp.exp2((scores - top) * scale)
        tops[p : p + 1, :] = top
        sums[p : p + 1, :] = jnp.sum(expo, axis=0, keepdims=True)
        total = dot(value[f], expo.astype(jnp.bfloat16), NN)
        outs[f.start : f.start + hdim, :] = total[:hdim, :rows]
        outs[f.start + hdim : f.stop, :] = total[hdim:, rows:]


def far_kernel(hdim, xa, xb, wown, wpair, pown, ppair, qcol, cosine, sine, *refs):
    scale = math.log2(math.e) / math.sqrt(hdim)
    near, (part, send, kout, vout) = (refs[:4], refs[4:8]), refs[8:]
    local = wown.shape[0] // 3
    rows = xa.shape[0]
    me = lax.axis_index("sp")
    normed = jnp.concatenate([xa[...], xb[...]], axis=0)
    cos, sin = cosine[:, 2 * rows :], sine[:, 2 * rows :]
    total = None
    for side, weight in enumerate((wown, wpair)):
        q, tops, sums, outs = near[side]
        owner = me ^ side
        base = slice(side * local, (side + 1) * local)
        keyval = dot(weight[local:, :], normed, NT)
        key = rotated(keyval[:local] + column(qcol, owner, local, 1), cos, sin, hdim)
        value = (keyval[local:] + column(qcol, owner, local, 2)).astype(jnp.bfloat16)
        kout[base, :] = key
        vout[base, :] = value
        pieces = []
        for p in range(local // (2 * hdim)):
            f = slice(2 * p * hdim, 2 * (p + 1) * hdim)
            scores = dot(key[f], q[f, :], TN)
            old = tops[p : p + 1, :]
            top = jnp.maximum(old, jnp.max(scores, axis=0, keepdims=True))
            expo = jnp.exp2((scores - top) * scale)
            shrink = jnp.exp2((old - top) * scale)
            inv = 1.0 / (sums[p : p + 1, :] * shrink + jnp.sum(expo, axis=0, keepdims=True))
            late = dot(value[f], expo.astype(jnp.bfloat16), NN)
            for h in range(2):
                lanes = slice(h * rows, (h + 1) * rows)
                feats = slice(h * hdim, (h + 1) * hdim)
                early = outs[f.start + h * hdim : f.start + (h + 1) * hdim, :]
                mixed = (early * shrink[:, lanes] + late[feats, lanes]) * inv[:, lanes]
                pieces.append(mixed.astype(jnp.bfloat16))
        add = dot(jnp.concatenate(pieces, axis=0), (pown, ppair)[side][...], TN)
        total = add if total is None else total + add
    part[...] = total
    send[...] = total.astype(jnp.bfloat16)


def late_kernel(hdim, x, wown, wpair, pown, ppair, qcol, cosine, sine, kna, vna, knb, vnb, kf, vf, part, send):
    scale = math.log2(math.e) / math.sqrt(hdim)
    local = wown.shape[0] // 3
    rows = x.shape[0]
    me = lax.axis_index("sp")
    total = None
    for side, weight in enumerate((wown, wpair)):
        query = dot(weight[:local, :], x[...], NT) + column(qcol, me ^ side, local, 0)
        far = slice(2 * rows, 3 * rows)
        query = paired(rotated(query, cosine[:, far], sine[:, far], hdim), hdim)
        pieces = []
        for at in range(0, local, 2 * hdim):
            f = slice(side * local + at, side * local + at + 2 * hdim)
            g = slice(at, at + 2 * hdim)
            kn, vn = ((kna, vna), (knb, vnb))[side]
            both = query[g]
            sn = dot(kn[g, :], both, TN)
            sf = dot(kf[f, :], both, TN)
            top = jnp.maximum(jnp.max(sn, axis=0, keepdims=True), jnp.max(sf, axis=0, keepdims=True))
            en = jnp.exp2((sn - top) * scale)
            ef = jnp.exp2((sf - top) * scale)
            inv = 1.0 / (jnp.sum(en, axis=0, keepdims=True) + jnp.sum(ef, axis=0, keepdims=True))
            mixed = dot(vn[g, :], (en * inv).astype(jnp.bfloat16), NN)
            mixed = (mixed + dot(vf[f, :], (ef * inv).astype(jnp.bfloat16), NN)).astype(jnp.bfloat16)
            pieces += [mixed[:hdim, :rows], mixed[hdim:, rows:]]
        add = dot(jnp.concatenate(pieces, axis=0), (pown, ppair)[side][...], TN)
        total = add if total is None else total + add
    part[...] = total
    send[...] = total.astype(jnp.bfloat16)


def merge_kernel(keep, x, part, got, rows, *rest):
    blocks, scratch = rest[-2], rest[-1]
    width = x.shape[1]
    value = x[...].astype(jnp.float32) + (part[...] + got[...].astype(jnp.float32)) + rows[2:3, :]
    rounded = value.astype(jnp.bfloat16)
    if keep:
        rest[-3][...] = rounded
    normed = layer_norm(rounded.astype(jnp.float32), rows[3:4, :], rows[4:5, :])
    count = x.shape[0] // 4
    lanes = scratch.shape[2]
    for t in range(width // lanes):
        scratch[t] = normed[:, t * lanes : (t + 1) * lanes]
        for j in range(4):
            at = j * width + t * lanes
            blocks[:, at : at + lanes] = scratch[t, pl.ds(j, count, stride=4), :].astype(jnp.bfloat16)


def gelu(v):
    return 0.5 * v * (1.0 + lax.erf(v * math.sqrt(0.5)))


def hidden_kernel(own, pair, weight, rows, out):
    core = lax.axis_index("sp") % 2
    count = own.shape[0]
    both = jnp.concatenate([own[...], pair[...]], axis=0)
    hid = gelu(dot(both, weight[...], NN) + rows[5:6, :]).astype(jnp.bfloat16)
    for half, place in enumerate((core, 1 - core)):
        out[pl.ds(pl.multiple_of(place * count, count), count), :] = hid[half * count : (half + 1) * count]


def last_kernel(own, pair, weight, rows, vit, early, out, vout, stage, sems):
    me = lax.axis_index("sp")
    chip, core = me // 2, me % 2
    count = own.shape[0]
    at = lambda start: pl.ds(pl.multiple_of(start, count), count)
    copies = [pltpu.make_async_copy(vit, vout, sems.at[0])]
    there = out.at[pl.ds(pl.multiple_of((1 - chip) * 2 * count, count), 2 * count)]
    copies.append(pltpu.make_async_copy(early, there, sems.at[1]))
    for copy in copies:
        copy.start()
    both = jnp.concatenate([own[...], pair[...]], axis=0)
    step = stage.shape[2]
    for n in range(stage.shape[0]):
        cols = slice(n * step, (n + 1) * step)
        stage[n] = gelu(dot(both, weight[:, cols], NN) + rows[5:6, cols]).astype(jnp.bfloat16)
        for half, place in enumerate((core, 1 - core)):
            copy = pltpu.make_async_copy(
                stage.at[n, pl.ds(half * count, count)],
                out.at[at(chip * 2 * count + place * count), pl.ds(n * step, step)],
                sems.at[2 + 2 * n + half],
            )
            copy.start()
            copies.append(copy)
    for copy in copies:
        copy.wait()


def shape(dims, dtype=jnp.bfloat16):
    return jax.ShapeDtypeStruct(dims, dtype)


def two_chips(
    patches,
    pos_ids,
    norm_gain,
    norm_bias,
    qkv_weight,
    qkv_bias,
    proj_weight,
    proj_bias,
    merge_gain,
    merge_bias,
    fc1_weight,
    fc1_bias,
):
    prow, width = patches.shape
    hdim = width // HEADS
    local = qkv_weight.shape[2]
    hidden = fc1_weight.shape[1]

    def swap(value, bit):
        return lax.ppermute(value, "sp", [(i, i ^ bit) for i in range(4)])

    weight = qkv_weight.transpose(1, 2, 0).reshape(3 * local, width)
    x_far = swap(patches, 2)
    x_pair = swap(patches, 1)
    w_pair = swap(weight, 1)
    p_pair = swap(proj_weight, 1)

    both = 2 * local
    part_shape = (shape((prow, width), jnp.float32), shape((prow, width)))
    mul = 2 * prow * width * local * 2
    table = shape((hdim // 2, 4 * prow), jnp.float32)

    sources = (patches, pos_ids, qkv_bias, norm_gain, norm_bias, proj_bias, merge_gain, merge_bias, fc1_bias)
    sources += (proj_weight, weight)
    held = lambda v: pltpu.VMEM(v.shape, v.dtype)
    x_own, w_own, p_own, n_own, rows, qcol, cos, sin = pl.pallas_call(
        functools.partial(setup_kernel, hdim, len(sources)),
        out_shape=(
            held(patches),
            held(weight),
            held(proj_weight),
            shape((prow, width)),
            shape((8, width), jnp.float32),
            shape((width, 8), jnp.float32),
            table,
            table,
        ),
        in_specs=[HBM] * len(sources),
        scratch_shapes=[held(v) for v in sources[1:-2]] + [pltpu.SemaphoreType.DMA((len(sources),))],
        compiler_params=pltpu.CompilerParams(vmem_limit_bytes=4 * MIB),
        cost_estimate=pl.CostEstimate(flops=mul, bytes_accessed=1 << 22, transcendentals=0),
        name="setup",
    )(*(pltpu.with_memory_space_constraint(v, pltpu.HBM) for v in sources))

    def norm(x, *after):
        return pl.pallas_call(
            norm_kernel,
            out_shape=shape((prow, width)),
            in_specs=[VMEM] * 2 + [ANY] * len(after),
            compiler_params=pltpu.CompilerParams(vmem_limit_bytes=4 * MIB),
            cost_estimate=pl.CostEstimate(flops=mul // 4, bytes_accessed=1 << 20, transcendentals=0),
        )(x, rows, *after)

    n_pair = norm(x_pair)
    flat = shape((local, 2 * prow))
    state = shape((local // (2 * hdim), 2 * prow), jnp.float32)
    near_shape = (flat, flat, flat, state, state, shape((local, prow), jnp.float32))

    def near(side, weight):
        q, k, v, *rest = call(
            functools.partial(near_kernel, hdim, side), near_shape, 8 * MIB, 4 * mul
        )(n_own, n_pair, weight, qcol, cos, sin)
        return (q, *rest), (k, v)

    early_own, kv_own = near(0, w_own)
    early_pair, kv_pair = near(1, w_pair)

    n_far = norm(x_far, early_own[1], early_pair[1])
    n_farpair = swap(n_far, 1)
    tall = shape((both, 2 * prow))
    shared = (w_own, w_pair, p_own, p_pair, qcol, cos, sin)
    part0, send0, k_far, v_far = call(
        functools.partial(far_kernel, hdim), part_shape + (tall, tall), 8 * MIB, 6 * mul
    )(n_far, n_farpair, *shared, *early_own, *early_pair)
    got1 = swap(send0, 2)
    part1, send1 = call(
        functools.partial(late_kernel, hdim), part_shape, 8 * MIB, 6 * mul
    )(n_far, *shared, *kv_own, *kv_pair, k_far, v_far)
    got0 = swap(send1, 2)
    late_rows = call(copy_kernel, shape(rows.shape, rows.dtype), MIB, 1000)(rows)

    blocks_shape = shape((prow // 4, 4 * width))

    def merge(x, part, got, outs, *after):
        return pl.pallas_call(
            functools.partial(merge_kernel, len(outs) == 2),
            out_shape=outs,
            in_specs=[VMEM] * 4 + [ANY] * len(after),
            scratch_shapes=[pltpu.VMEM((width // 128, prow, 128), jnp.float32)],
            compiler_params=pltpu.CompilerParams(vmem_limit_bytes=4 * MIB),
            cost_estimate=pl.CostEstimate(flops=mul // 4, bytes_accessed=1 << 20, transcendentals=0),
        )(x, part, got, late_rows, *after)

    fc1 = pltpu.with_memory_space_constraint(fc1_weight, pltpu.VMEM)
    (blocks1,) = merge(x_far, part1, got1, (blocks_shape,))
    pair1 = swap(blocks1, 1)
    flops = prow * 4 * width * hidden
    early = call(hidden_kernel, shape((prow // 2, hidden)), 4 * MIB, flops)(blocks1, pair1, fc1, rows)
    vit, blocks0 = merge(x_own, part0, got0, (shape((prow, width)), blocks_shape), early)
    pair0 = swap(blocks0, 1)
    parts = hidden // 256
    merged, vit_out = pl.pallas_call(
        last_kernel,
        out_shape=(shape((prow, hidden)), shape((prow, width))),
        out_specs=[HBM] * 2,
        scratch_shapes=[
            pltpu.VMEM((parts, prow // 2, 256), jnp.bfloat16),
            pltpu.SemaphoreType.DMA((2 + 2 * parts,)),
        ],
        compiler_params=pltpu.CompilerParams(vmem_limit_bytes=4 * MIB),
        cost_estimate=pl.CostEstimate(flops=flops, bytes_accessed=1 << 24, transcendentals=0),
        name="hidden0",
    )(blocks0, pair0, fc1, rows, vit, early)
    return vit_out, merged


def rotate(values, positions, nheads):
    count = values.shape[0]
    hdim = values.shape[1] // nheads
    quarter = hdim // 4
    inv = 1.0 / 10000.0 ** (jnp.arange(quarter, dtype=jnp.float32) * 2.0 / (hdim // 2))
    rows = positions[0].astype(jnp.float32)[:, None] * inv
    cols = positions[1].astype(jnp.float32)[:, None] * inv
    angle = jnp.concatenate([rows, cols, rows, cols], axis=1)
    cosine = jnp.cos(angle)[:, None, :]
    sine = jnp.sin(angle)[:, None, :]
    shaped = values.reshape(count, nheads, hdim)
    half = hdim // 2
    turned = jnp.concatenate([-shaped[..., half:], shaped[..., :half]], axis=-1)
    return (shaped * cosine + turned * sine).reshape(count, nheads * hdim)


def attend_blocks(query, keys, value, nheads, hdim):
    count = query.shape[0]
    block = min(512, count)
    qblocks = query.reshape(count // block, block, nheads, hdim)
    kshaped = keys.reshape(count, nheads, hdim)
    vshaped = value.reshape(count, nheads, hdim)
    scale = 1.0 / jnp.sqrt(jnp.float32(hdim))

    def one_block(qpart):
        scores = jnp.einsum("bhd,khd->hbk", qpart, kshaped, preferred_element_type=jnp.float32) * scale
        top = jnp.max(scores, axis=-1, keepdims=True)
        expo = jnp.exp(scores - top)
        weights = (expo / jnp.sum(expo, axis=-1, keepdims=True)).astype(jnp.bfloat16)
        result = jnp.einsum("hbk,khd->bhd", weights, vshaped, preferred_element_type=jnp.float32)
        return result.astype(jnp.bfloat16).reshape(block, nheads * hdim)

    return lax.map(one_block, qblocks).reshape(count, nheads * hdim)


def any_size(
    patches,
    pos_ids,
    norm_gain,
    norm_bias,
    qkv_weight,
    qkv_bias,
    proj_weight,
    proj_bias,
    merge_gain,
    merge_bias,
    fc1_weight,
    fc1_bias,
):
    groups = lax.axis_size("sp")
    where = lax.axis_index("sp")
    prow, width = patches.shape
    heads_local = HEADS // groups
    hdim = width // HEADS
    local_width = width // groups
    xfloat = patches.astype(jnp.float32)
    normed = layer_norm(xfloat, norm_gain, norm_bias).astype(jnp.bfloat16)
    bias_local = lax.dynamic_slice_in_dim(qkv_bias, where * local_width, local_width, 1)
    qkv = (
        jnp.einsum(
            "pd,dcn->pcn",
            lax.all_gather(normed, "sp", axis=0, tiled=True),
            qkv_weight,
            preferred_element_type=jnp.float32,
        )
        + bias_local[None]
    )
    query = rotate(qkv[:, 0], pos_ids, heads_local).astype(jnp.bfloat16)
    keys = rotate(qkv[:, 1], pos_ids, heads_local).astype(jnp.bfloat16)
    value = qkv[:, 2].astype(jnp.bfloat16)
    attended = attend_blocks(query, keys, value, heads_local, hdim)
    returned = lax.all_to_all(attended, "sp", split_axis=0, concat_axis=1, tiled=True)
    projected = jnp.dot(
        returned,
        lax.all_gather(proj_weight, "sp", axis=0, tiled=True),
        preferred_element_type=jnp.float32,
    )
    vit_out = (xfloat + projected + proj_bias).astype(jnp.bfloat16)
    zn = layer_norm(vit_out.astype(jnp.float32), merge_gain, merge_bias).astype(jnp.bfloat16)
    blocks = zn.reshape(prow // 4, 4 * width)
    hidden = (
        jnp.dot(
            lax.all_gather(blocks, "sp", axis=0, tiled=True),
            fc1_weight,
            preferred_element_type=jnp.float32,
        )
        + fc1_bias
    )
    merged_hidden = jax.nn.gelu(hidden, approximate=False).astype(jnp.bfloat16)
    return (vit_out, merged_hidden)


def per_device(*args):
    if lax.axis_size("sp") == 4:
        return two_chips(*args)
    return any_size(*args)


def solution(mesh):
    return jax.shard_map(
        per_device,
        mesh=mesh,
        in_specs=(
            P(("img", "sp"), None),
            P(None, "img"),
            P(),
            P(),
            P(None, None, "sp"),
            P(),
            P("sp", None),
            P(),
            P(),
            P(),
            P(None, "sp"),
            P("sp"),
        ),
        out_specs=(P(("img", "sp"), None), P("img", "sp")),
        check_vma=False,
    )
```

```python
import functools
import math

import jax
import jax.numpy as jnp
from jax import lax
from jax.experimental import pallas as pl
from jax.experimental.pallas import tpu as pltpu
from jax.sharding import PartitionSpec as P


HEADS = 16
EPS = 1e-06
MIB = 1 << 20
VMEM = pl.BlockSpec(memory_space=pltpu.VMEM)
ANY = pl.BlockSpec(memory_space=pl.ANY)
HBM = pl.BlockSpec(memory_space=pltpu.HBM)
NT = (((1,), (1,)), ((), ()))
TN = (((0,), (0,)), ((), ()))
NN = (((1,), (0,)), ((), ()))


def layer_norm(values, gain, bias):
    mean = jnp.mean(values, axis=-1, keepdims=True)
    centered = values - mean
    var = jnp.mean(centered * centered, axis=-1, keepdims=True)
    return centered * lax.rsqrt(var + EPS) * gain + bias


def dot(a, b, dims):
    return lax.dot_general(a, b, dims, preferred_element_type=jnp.float32)


def call(kernel, outs, nbytes, flops):
    return pl.pallas_call(
        kernel,
        out_shape=outs,
        compiler_params=pltpu.CompilerParams(vmem_limit_bytes=nbytes),
        cost_estimate=pl.CostEstimate(flops=flops, bytes_accessed=1 << 20, transcendentals=0),
    )


def setup_kernel(hdim, count, *refs):
    sources, rest = refs[:count], refs[count:]
    x, wown, pall, normed, rows, qcol, cosine, sine, pos, qkv_bias = rest[:10]
    vectors, sems = rest[10:-1], rest[-1]
    targets = (x, pos, qkv_bias) + tuple(vectors) + (pall.at[pl.ds(0, pall.shape[0] // 2)], wown)
    copies = [pltpu.make_async_copy(a, b, sems.at[n]) for n, (a, b) in enumerate(zip(sources, targets))]
    for copy in copies:
        copy.start()
    prow, width = x.shape
    me = lax.axis_index("sp")
    quarter = hdim // 4
    feature = lax.broadcasted_iota(jnp.int32, (2 * quarter, prow), 0)
    second = feature >= quarter
    power = jnp.where(second, feature - quarter, feature).astype(jnp.float32)
    inv = jnp.exp(power * (-2.0 * math.log(10000.0) / (hdim // 2)))
    rows[...] = jnp.zeros_like(rows)
    for copy in copies[:-2]:
        copy.wait()
    for k in range(4):
        at = pl.ds(pl.multiple_of((me ^ k) * prow, prow), prow)
        place = jnp.where(second, pos[1:2, at], pos[0:1, at]).astype(jnp.float32)
        angle = place * inv
        cosine[:, k * prow : (k + 1) * prow] = jnp.cos(angle)
        sine[:, k * prow : (k + 1) * prow] = jnp.sin(angle)
    for at, vector in enumerate(vectors):
        rows[at : at + 1, :] = vector[...].reshape(1, width)
    cube = jnp.concatenate([qkv_bias[...], jnp.zeros((5, width), jnp.float32)], axis=0)
    qcol[...] = cube.T
    value = layer_norm(x[...].astype(jnp.float32), rows[0:1, :], rows[1:2, :])
    normed[...] = value.astype(jnp.bfloat16)
    for copy in copies[-2:]:
        copy.wait()


def copy_kernel(x, out):
    out[...] = x[...]


def norm_kernel(start, x, rows, *rest):
    out = rest[-1]
    value = x[start : start + out.shape[0], :].astype(jnp.float32)
    out[...] = layer_norm(value, rows[0:1, :], rows[1:2, :]).astype(jnp.bfloat16)


def column(qcol, owner, local, c):
    return qcol[pl.ds(pl.multiple_of(owner * local, 8), local), c : c + 1]


def rotated(raw, cos, sin, hdim):
    half = hdim // 2
    pieces = []
    for at in range(0, raw.shape[0], hdim):
        top, low = raw[at : at + half], raw[at + half : at + hdim]
        pieces += [top * cos - low * sin, low * cos + top * sin]
    return jnp.concatenate(pieces, axis=0).astype(jnp.bfloat16)


def paired(query, hdim):
    zero = jnp.zeros((hdim, query.shape[1]), query.dtype)
    rows = []
    for at in range(0, query.shape[0], 2 * hdim):
        rows.append(jnp.concatenate([query[at : at + hdim], zero], axis=1))
        rows.append(jnp.concatenate([zero, query[at + hdim : at + 2 * hdim]], axis=1))
    return jnp.concatenate(rows, axis=0)


def near_kernel(hdim, side, xa, xb, weight, qcol, cosine, sine, *rest):
    if side:
        ppair, _, qout, kout, vout, tops, sums, outs, pall, sem = rest
        count = ppair.shape[0]
        copy = pltpu.make_async_copy(ppair, pall.at[pl.ds(count, count)], sem)
        copy.start()
    else:
        qout, kout, vout, tops, sums, outs = rest
    scale = math.log2(math.e) / math.sqrt(hdim)
    local = weight.shape[0] // 3
    rows = xa.shape[0]
    owner = lax.axis_index("sp") ^ side
    normed = jnp.concatenate([xa[...], xb[...]], axis=0)
    cos, sin = cosine[:, : 2 * rows], sine[:, : 2 * rows]
    query = dot(weight[0:local, :], normed[:rows], NT) + column(qcol, owner, local, 0)
    query = paired(rotated(query, cos[:, :rows], sin[:, :rows], hdim), hdim)
    keyval = dot(weight[local:, :], normed, NT)
    key = rotated(keyval[:local] + column(qcol, owner, local, 1), cos, sin, hdim)
    value = (keyval[local:] + column(qcol, owner, local, 2)).astype(jnp.bfloat16)
    qout[...] = query
    kout[...] = key
    vout[...] = value
    for p in range(local // (2 * hdim)):
        f = slice(2 * p * hdim, 2 * (p + 1) * hdim)
        scores = dot(key[f], query[f], TN)
        top = jnp.max(scores, axis=0, keepdims=True)
        expo = jnp.exp2((scores - top) * scale)
        tops[p : p + 1, :] = top
        sums[p : p + 1, :] = jnp.sum(expo, axis=0, keepdims=True)
        total = dot(value[f], expo.astype(jnp.bfloat16), NN)
        outs[f.start : f.start + hdim, :] = total[:hdim, :rows]
        outs[f.start + hdim : f.stop, :] = total[hdim:, rows:]
    if side:
        copy.wait()


def far_kernel(hdim, xa, xb, xc, xd, wown, wpair, pall, qcol, cosine, sine, *refs):
    scale = math.log2(math.e) / math.sqrt(hdim)
    near, (part, send, kout, vout) = (refs[:4], refs[4:8]), refs[8:]
    local = wown.shape[0] // 3
    rows = 2 * xa.shape[0]
    me = lax.axis_index("sp")
    normed = jnp.concatenate([x[...] for x in (xa, xb, xc, xd)], axis=0)
    cos, sin = cosine[:, 2 * rows :], sine[:, 2 * rows :]
    for side, weight in enumerate((wown, wpair)):
        owner = me ^ side
        base = slice(side * local, (side + 1) * local)
        keyval = dot(weight[local:, :], normed, NT)
        kout[base, :] = rotated(keyval[:local] + column(qcol, owner, local, 1), cos, sin, hdim)
        vout[base, :] = (keyval[local:] + column(qcol, owner, local, 2)).astype(jnp.bfloat16)
    pieces = []
    for side in range(2):
        q, tops, sums, outs = near[side]
        for p in range(local // (2 * hdim)):
            f = slice(2 * p * hdim, 2 * (p + 1) * hdim)
            g = slice(side * local + f.start, side * local + f.stop)
            scores = dot(kout[g, :], q[f, :], TN)
            old = tops[p : p + 1, :]
            top = jnp.maximum(old, jnp.max(scores, axis=0, keepdims=True))
            expo = jnp.exp2((scores - top) * scale)
            shrink = jnp.exp2((old - top) * scale)
            inv = 1.0 / (sums[p : p + 1, :] * shrink + jnp.sum(expo, axis=0, keepdims=True))
            late = dot(vout[g, :], expo.astype(jnp.bfloat16), NN)
            for h in range(2):
                lanes = slice(h * rows, (h + 1) * rows)
                feats = slice(h * hdim, (h + 1) * hdim)
                early = outs[f.start + h * hdim : f.start + (h + 1) * hdim, :]
                mixed = (early * shrink[:, lanes] + late[feats, lanes]) * inv[:, lanes]
                pieces.append(mixed.astype(jnp.bfloat16))
    total = dot(jnp.concatenate(pieces, axis=0), pall[...], TN)
    part[...] = total
    send[...] = total.astype(jnp.bfloat16)


def late_kernel(hdim, xa, xb, wown, wpair, pall, qcol, cosine, sine, kna, vna, knb, vnb, kf, vf, part, send0, send1):
    scale = math.log2(math.e) / math.sqrt(hdim)
    local = wown.shape[0] // 3
    rows = 2 * xa.shape[0]
    me = lax.axis_index("sp")
    normed = jnp.concatenate([xa[...], xb[...]], axis=0)
    pieces = []
    for side, weight in enumerate((wown, wpair)):
        query = dot(weight[:local, :], normed, NT) + column(qcol, me ^ side, local, 0)
        far = slice(2 * rows, 3 * rows)
        query = paired(rotated(query, cosine[:, far], sine[:, far], hdim), hdim)
        for at in range(0, local, 2 * hdim):
            f = slice(side * local + at, side * local + at + 2 * hdim)
            g = slice(at, at + 2 * hdim)
            kn, vn = ((kna, vna), (knb, vnb))[side]
            both = query[g]
            sn = dot(kn[g, :], both, TN)
            sf = dot(kf[f, :], both, TN)
            top = jnp.maximum(jnp.max(sn, axis=0, keepdims=True), jnp.max(sf, axis=0, keepdims=True))
            en = jnp.exp2((sn - top) * scale)
            ef = jnp.exp2((sf - top) * scale)
            inv = 1.0 / (jnp.sum(en, axis=0, keepdims=True) + jnp.sum(ef, axis=0, keepdims=True))
            mixed = dot(vn[g, :], (en * inv).astype(jnp.bfloat16), NN)
            mixed = (mixed + dot(vf[f, :], (ef * inv).astype(jnp.bfloat16), NN)).astype(jnp.bfloat16)
            pieces += [mixed[:hdim, :rows], mixed[hdim:, rows:]]
    total = dot(jnp.concatenate(pieces, axis=0), pall[...], TN)
    part[...] = total
    half = rows // 2
    send0[...] = total[:half].astype(jnp.bfloat16)
    send1[...] = total[half:].astype(jnp.bfloat16)


def merge_kernel(keep, start, x, part, got, rows, *rest):
    blocks, scratch = rest[-2], rest[-1]
    width = x.shape[1]
    place = slice(start, start + got.shape[0])
    value = x[place, :].astype(jnp.float32) + (part[place, :] + got[...].astype(jnp.float32)) + rows[2:3, :]
    rounded = value.astype(jnp.bfloat16)
    if keep:
        rest[-3][...] = rounded
    normed = layer_norm(rounded.astype(jnp.float32), rows[3:4, :], rows[4:5, :])
    count = got.shape[0] // 4
    lanes = scratch.shape[2]
    for t in range(width // lanes):
        scratch[t] = normed[:, t * lanes : (t + 1) * lanes]
        for j in range(4):
            at = j * width + t * lanes
            blocks[:, at : at + lanes] = scratch[t, pl.ds(j, count, stride=4), :].astype(jnp.bfloat16)


def gelu(v):
    return 0.5 * v * (1.0 + lax.erf(v * math.sqrt(0.5)))


def hidden_kernel(own, pair, weight, rows, out):
    core = lax.axis_index("sp") % 2
    count = own.shape[0]
    both = jnp.concatenate([own[...], pair[...]] * 2, axis=0)
    hid = gelu(dot(both, weight[...], NN)[: 2 * count] + rows[5:6, :]).astype(jnp.bfloat16)
    for half, place in enumerate((core, 1 - core)):
        out[pl.ds(pl.multiple_of(place * count, count), count), :] = hid[half * count : (half + 1) * count]


def last_kernel(own0, own1, pair0, pair1, weight, rows, vit0, vit1, early, out, vout, stage, sems):
    me = lax.axis_index("sp")
    chip, core = me // 2, me % 2
    count = 2 * own0.shape[0]
    half = vit0.shape[0]
    at = lambda start: pl.ds(pl.multiple_of(start, count), count)
    there = out.at[pl.ds(pl.multiple_of((1 - chip) * 2 * count, count), 2 * count)]
    copies = [
        pltpu.make_async_copy(vit0, vout.at[pl.ds(0, half)], sems.at[0]),
        pltpu.make_async_copy(vit1, vout.at[pl.ds(half, half)], sems.at[1]),
        pltpu.make_async_copy(early, there, sems.at[2]),
    ]
    for copy in copies:
        copy.start()
    both = jnp.concatenate([x[...] for x in (own0, own1, pair0, pair1)] * 2, axis=0)
    step = stage.shape[2]
    for n in range(stage.shape[0]):
        cols = slice(n * step, (n + 1) * step)
        value = dot(both, weight[:, cols], NN)[: 2 * count] + rows[5:6, cols]
        stage[n] = gelu(value).astype(jnp.bfloat16)
        for side, place in enumerate((core, 1 - core)):
            copy = pltpu.make_async_copy(
                stage.at[n, pl.ds(side * count, count)],
                out.at[at(chip * 2 * count + place * count), pl.ds(n * step, step)],
                sems.at[3 + 2 * n + side],
            )
            copy.start()
            copies.append(copy)
    for copy in copies:
        copy.wait()


def shape(dims, dtype=jnp.bfloat16):
    return jax.ShapeDtypeStruct(dims, dtype)


def two_chips(
    patches,
    pos_ids,
    norm_gain,
    norm_bias,
    qkv_weight,
    qkv_bias,
    proj_weight,
    proj_bias,
    merge_gain,
    merge_bias,
    fc1_weight,
    fc1_bias,
):
    prow, width = patches.shape
    hdim = width // HEADS
    local = qkv_weight.shape[2]
    hidden = fc1_weight.shape[1]

    def swap(value, bit):
        return lax.ppermute(value, "sp", [(i, i ^ bit) for i in range(4)])

    weight = qkv_weight.transpose(1, 2, 0).reshape(3 * local, width)
    x_far = swap(patches, 2)
    x_pair = swap(patches, 1)
    w_pair = swap(weight, 1)
    p_pair = swap(proj_weight, 1)

    both = 2 * local
    mul = 2 * prow * width * local * 2
    table = shape((hdim // 2, 4 * prow), jnp.float32)

    sources = (patches, pos_ids, qkv_bias, norm_gain, norm_bias, proj_bias, merge_gain, merge_bias, fc1_bias)
    sources += (proj_weight, weight)
    held = lambda v: pltpu.VMEM(v.shape, v.dtype)
    x_own, w_own, p_half, n_own, rows, qcol, cos, sin = pl.pallas_call(
        functools.partial(setup_kernel, hdim, len(sources)),
        out_shape=(
            held(patches),
            held(weight),
            pltpu.VMEM((both, width), proj_weight.dtype),
            shape((prow, width)),
            shape((8, width), jnp.float32),
            shape((width, 8), jnp.float32),
            table,
            table,
        ),
        in_specs=[HBM] * len(sources),
        scratch_shapes=[held(v) for v in sources[1:-2]] + [pltpu.SemaphoreType.DMA((len(sources),))],
        compiler_params=pltpu.CompilerParams(vmem_limit_bytes=4 * MIB),
        cost_estimate=pl.CostEstimate(flops=mul, bytes_accessed=1 << 22, transcendentals=0),
        name="setup",
    )(*(pltpu.with_memory_space_constraint(v, pltpu.HBM) for v in sources))

    def norm(x, start, count, *after):
        return pl.pallas_call(
            functools.partial(norm_kernel, start),
            out_shape=shape((count, width)),
            in_specs=[VMEM] * 2 + [ANY] * len(after),
            compiler_params=pltpu.CompilerParams(vmem_limit_bytes=4 * MIB),
            cost_estimate=pl.CostEstimate(flops=mul // 4, bytes_accessed=1 << 20, transcendentals=0),
        )(x, rows, *after)

    n_pair = norm(x_pair, 0, prow)
    flat = shape((local, 2 * prow))
    state = shape((local // (2 * hdim), 2 * prow), jnp.float32)
    near_shape = (flat, flat, flat, state, state, shape((local, prow), jnp.float32))

    def near(side, weight, *more):
        return pl.pallas_call(
            functools.partial(near_kernel, hdim, side),
            out_shape=near_shape + (pltpu.VMEM((both, width), proj_weight.dtype),) * side,
            input_output_aliases={7: 6} if side else {},
            scratch_shapes=[pltpu.SemaphoreType.DMA] * side,
            compiler_params=pltpu.CompilerParams(vmem_limit_bytes=8 * MIB),
            cost_estimate=pl.CostEstimate(flops=4 * mul, bytes_accessed=1 << 22, transcendentals=0),
        )(n_own, n_pair, weight, qcol, cos, sin, *more)

    q, *kv_own, tops, sums, outs = near(0, w_own)
    early_own = (q, tops, sums, outs)
    q, *kv_pair, tops, sums, outs, p_all = near(1, w_pair, p_pair, p_half)
    early_pair = (q, tops, sums, outs)

    half = prow // 2
    n_far0 = norm(x_far, 0, half, early_own[1], p_all)
    n_farpair0 = swap(n_far0, 1)
    n_far1 = norm(x_far, half, half, n_far0)
    n_farpair1 = swap(n_far1, 1)
    tall = shape((both, 2 * prow))
    shared = (w_own, w_pair, p_all, qcol, cos, sin)
    part_shape = shape((prow, width), jnp.float32)
    part0, send0, k_far, v_far = call(
        functools.partial(far_kernel, hdim), (part_shape, shape((prow, width)), tall, tall), 8 * MIB, 6 * mul
    )(n_far0, n_far1, n_farpair0, n_farpair1, *shared, *early_own, *early_pair)
    got1 = swap(send0, 2)
    halves = (shape((half, width)), shape((half, width)))
    part1, send1a, send1b = call(
        functools.partial(late_kernel, hdim), (part_shape,) + halves, 8 * MIB, 6 * mul
    )(n_far0, n_far1, *shared, *kv_own, *kv_pair, k_far, v_far)
    got0a = swap(send1a, 2)
    got0b = swap(send1b, 2)
    late_rows = call(copy_kernel, shape(rows.shape, rows.dtype), MIB, 1000)(rows)

    def merge(keep, start, x, part, got, late_rows, *after):
        count = got.shape[0]
        outs = (shape((count, width)),) * keep + (shape((count // 4, 4 * width)),)
        return pl.pallas_call(
            functools.partial(merge_kernel, keep, start),
            out_shape=outs,
            in_specs=[VMEM] * 4 + [ANY] * len(after),
            scratch_shapes=[pltpu.VMEM((width // 128, count, 128), jnp.float32)],
            compiler_params=pltpu.CompilerParams(vmem_limit_bytes=4 * MIB),
            cost_estimate=pl.CostEstimate(flops=mul // 4, bytes_accessed=1 << 20, transcendentals=0),
        )(x, part, got, late_rows, *after)

    fc1 = pltpu.with_memory_space_constraint(fc1_weight, pltpu.VMEM)
    (blocks1,) = merge(0, 0, x_far, part1, got1, late_rows)
    pair1 = swap(blocks1, 1)
    flops = prow * 4 * width * hidden
    early = call(hidden_kernel, shape((prow // 2, hidden)), 4 * MIB, flops)(blocks1, pair1, fc1, rows)
    vit_a, blocks_a = merge(1, 0, x_own, part0, got0a, late_rows, early)
    pair_a = swap(blocks_a, 1)
    late_rows = call(copy_kernel, shape(rows.shape, rows.dtype), MIB, 1000)(late_rows)
    vit_b, blocks_b = merge(1, half, x_own, part0, got0b, late_rows)
    pair_b = swap(blocks_b, 1)
    parts = hidden // 256
    merged, vit_out = pl.pallas_call(
        last_kernel,
        out_shape=(shape((prow, hidden)), shape((prow, width))),
        out_specs=[HBM] * 2,
        scratch_shapes=[
            pltpu.VMEM((parts, prow // 2, 256), jnp.bfloat16),
            pltpu.SemaphoreType.DMA((3 + 2 * parts,)),
        ],
        compiler_params=pltpu.CompilerParams(vmem_limit_bytes=4 * MIB),
        cost_estimate=pl.CostEstimate(flops=flops, bytes_accessed=1 << 24, transcendentals=0),
        name="hidden0",
    )(blocks_a, blocks_b, pair_a, pair_b, fc1, rows, vit_a, vit_b, early)
    return vit_out, merged


def rotate(values, positions, nheads):
    count = values.shape[0]
    hdim = values.shape[1] // nheads
    quarter = hdim // 4
    inv = 1.0 / 10000.0 ** (jnp.arange(quarter, dtype=jnp.float32) * 2.0 / (hdim // 2))
    rows = positions[0].astype(jnp.float32)[:, None] * inv
    cols = positions[1].astype(jnp.float32)[:, None] * inv
    angle = jnp.concatenate([rows, cols, rows, cols], axis=1)
    cosine = jnp.cos(angle)[:, None, :]
    sine = jnp.sin(angle)[:, None, :]
    shaped = values.reshape(count, nheads, hdim)
    half = hdim // 2
    turned = jnp.concatenate([-shaped[..., half:], shaped[..., :half]], axis=-1)
    return (shaped * cosine + turned * sine).reshape(count, nheads * hdim)


def attend_blocks(query, keys, value, nheads, hdim):
    count = query.shape[0]
    block = min(512, count)
    qblocks = query.reshape(count // block, block, nheads, hdim)
    kshaped = keys.reshape(count, nheads, hdim)
    vshaped = value.reshape(count, nheads, hdim)
    scale = 1.0 / jnp.sqrt(jnp.float32(hdim))

    def one_block(qpart):
        scores = jnp.einsum("bhd,khd->hbk", qpart, kshaped, preferred_element_type=jnp.float32) * scale
        top = jnp.max(scores, axis=-1, keepdims=True)
        expo = jnp.exp(scores - top)
        weights = (expo / jnp.sum(expo, axis=-1, keepdims=True)).astype(jnp.bfloat16)
        result = jnp.einsum("hbk,khd->bhd", weights, vshaped, preferred_element_type=jnp.float32)
        return result.astype(jnp.bfloat16).reshape(block, nheads * hdim)

    return lax.map(one_block, qblocks).reshape(count, nheads * hdim)


def any_size(
    patches,
    pos_ids,
    norm_gain,
    norm_bias,
    qkv_weight,
    qkv_bias,
    proj_weight,
    proj_bias,
    merge_gain,
    merge_bias,
    fc1_weight,
    fc1_bias,
):
    groups = lax.axis_size("sp")
    where = lax.axis_index("sp")
    prow, width = patches.shape
    heads_local = HEADS // groups
    hdim = width // HEADS
    local_width = width // groups
    xfloat = patches.astype(jnp.float32)
    normed = layer_norm(xfloat, norm_gain, norm_bias).astype(jnp.bfloat16)
    bias_local = lax.dynamic_slice_in_dim(qkv_bias, where * local_width, local_width, 1)
    qkv = (
        jnp.einsum(
            "pd,dcn->pcn",
            lax.all_gather(normed, "sp", axis=0, tiled=True),
            qkv_weight,
            preferred_element_type=jnp.float32,
        )
        + bias_local[None]
    )
    query = rotate(qkv[:, 0], pos_ids, heads_local).astype(jnp.bfloat16)
    keys = rotate(qkv[:, 1], pos_ids, heads_local).astype(jnp.bfloat16)
    value = qkv[:, 2].astype(jnp.bfloat16)
    attended = attend_blocks(query, keys, value, heads_local, hdim)
    returned = lax.all_to_all(attended, "sp", split_axis=0, concat_axis=1, tiled=True)
    projected = jnp.dot(
        returned,
        lax.all_gather(proj_weight, "sp", axis=0, tiled=True),
        preferred_element_type=jnp.float32,
    )
    vit_out = (xfloat + projected + proj_bias).astype(jnp.bfloat16)
    zn = layer_norm(vit_out.astype(jnp.float32), merge_gain, merge_bias).astype(jnp.bfloat16)
    blocks = zn.reshape(prow // 4, 4 * width)
    hidden = (
        jnp.dot(
            lax.all_gather(blocks, "sp", axis=0, tiled=True),
            fc1_weight,
            preferred_element_type=jnp.float32,
        )
        + fc1_bias
    )
    merged_hidden = jax.nn.gelu(hidden, approximate=False).astype(jnp.bfloat16)
    return (vit_out, merged_hidden)


def per_device(*args):
    if lax.axis_size("sp") == 4:
        return two_chips(*args)
    return any_size(*args)


def solution(mesh):
    return jax.shard_map(
        per_device,
        mesh=mesh,
        in_specs=(
            P(("img", "sp"), None),
            P(None, "img"),
            P(),
            P(),
            P(None, None, "sp"),
            P(),
            P("sp", None),
            P(),
            P(),
            P(),
            P(None, "sp"),
            P("sp"),
        ),
        out_specs=(P(("img", "sp"), None), P("img", "sp")),
        check_vma=False,
    )
```

```python
import functools
import math

import jax
import jax.numpy as jnp
from jax import lax
from jax.experimental import pallas as pl
from jax.experimental.pallas import tpu as pltpu
from jax.sharding import PartitionSpec as P


HEADS = 16
EPS = 1e-06
MIB = 1 << 20
VMEM = pl.BlockSpec(memory_space=pltpu.VMEM)
ANY = pl.BlockSpec(memory_space=pl.ANY)
HBM = pl.BlockSpec(memory_space=pltpu.HBM)
NT = (((1,), (1,)), ((), ()))
TN = (((0,), (0,)), ((), ()))
NN = (((1,), (0,)), ((), ()))


def layer_norm(values, gain, bias):
    mean = jnp.mean(values, axis=-1, keepdims=True)
    centered = values - mean
    var = jnp.mean(centered * centered, axis=-1, keepdims=True)
    return centered * lax.rsqrt(var + EPS) * gain + bias


def dot(a, b, dims):
    return lax.dot_general(a, b, dims, preferred_element_type=jnp.float32)


def call(kernel, outs, nbytes, flops):
    return pl.pallas_call(
        kernel,
        out_shape=outs,
        compiler_params=pltpu.CompilerParams(vmem_limit_bytes=nbytes),
        cost_estimate=pl.CostEstimate(flops=flops, bytes_accessed=1 << 20, transcendentals=0),
    )


def setup_kernel(hdim, count, *refs):
    sources, rest = refs[:count], refs[count:]
    x, wown, pall, normed, rows, qcol, cosine, sine, pos, qkv_bias = rest[:10]
    vectors, sems = rest[10:-1], rest[-1]
    targets = (x, pos, qkv_bias) + tuple(vectors) + (pall.at[pl.ds(0, pall.shape[0] // 2)], wown)
    copies = [pltpu.make_async_copy(a, b, sems.at[n]) for n, (a, b) in enumerate(zip(sources, targets))]
    for copy in copies:
        copy.start()
    prow, width = x.shape
    me = lax.axis_index("sp")
    quarter = hdim // 4
    feature = lax.broadcasted_iota(jnp.int32, (2 * quarter, prow), 0)
    second = feature >= quarter
    power = jnp.where(second, feature - quarter, feature).astype(jnp.float32)
    inv = jnp.exp(power * (-2.0 * math.log(10000.0) / (hdim // 2)))
    rows[...] = jnp.zeros_like(rows)
    for copy in copies[:-2]:
        copy.wait()
    for k in range(4):
        at = pl.ds(pl.multiple_of((me ^ k) * prow, prow), prow)
        place = jnp.where(second, pos[1:2, at], pos[0:1, at]).astype(jnp.float32)
        angle = place * inv
        cosine[:, k * prow : (k + 1) * prow] = jnp.cos(angle)
        sine[:, k * prow : (k + 1) * prow] = jnp.sin(angle)
    for at, vector in enumerate(vectors):
        rows[at : at + 1, :] = vector[...].reshape(1, width)
    cube = jnp.concatenate([qkv_bias[...], jnp.zeros((5, width), jnp.float32)], axis=0)
    qcol[...] = cube.T
    value = layer_norm(x[...].astype(jnp.float32), rows[0:1, :], rows[1:2, :])
    normed[...] = value.astype(jnp.bfloat16)
    for copy in copies[-2:]:
        copy.wait()


def copy_kernel(x, out):
    out[...] = x[...]


def norm_kernel(start, x, rows, *rest):
    out = rest[-1]
    value = x[start : start + out.shape[0], :].astype(jnp.float32)
    out[...] = layer_norm(value, rows[0:1, :], rows[1:2, :]).astype(jnp.bfloat16)


def column(qcol, owner, local, c):
    return qcol[pl.ds(pl.multiple_of(owner * local, 8), local), c : c + 1]


def rotated(raw, cos, sin, hdim):
    half = hdim // 2
    pieces = []
    for at in range(0, raw.shape[0], hdim):
        top, low = raw[at : at + half], raw[at + half : at + hdim]
        pieces += [top * cos - low * sin, low * cos + top * sin]
    return jnp.concatenate(pieces, axis=0).astype(jnp.bfloat16)


def paired(query, hdim):
    zero = jnp.zeros((hdim, query.shape[1]), query.dtype)
    rows = []
    for at in range(0, query.shape[0], 2 * hdim):
        rows.append(jnp.concatenate([query[at : at + hdim], zero], axis=1))
        rows.append(jnp.concatenate([zero, query[at + hdim : at + 2 * hdim]], axis=1))
    return jnp.concatenate(rows, axis=0)


def near_kernel(hdim, side, xa, xb, weight, qcol, cosine, sine, *rest):
    if side:
        ppair, _, qout, kout, vout, tops, sums, outs, pall, sem = rest
        count = ppair.shape[0]
        copy = pltpu.make_async_copy(ppair, pall.at[pl.ds(count, count)], sem)
        copy.start()
    else:
        qout, kout, vout, tops, sums, outs = rest
    scale = math.log2(math.e) / math.sqrt(hdim)
    local = weight.shape[0] // 3
    rows = xa.shape[0]
    owner = lax.axis_index("sp") ^ side
    normed = jnp.concatenate([xa[...], xb[...]], axis=0)
    cos, sin = cosine[:, : 2 * rows], sine[:, : 2 * rows]
    query = dot(weight[0:local, :], normed[:rows], NT) + column(qcol, owner, local, 0)
    query = paired(rotated(query, cos[:, :rows], sin[:, :rows], hdim), hdim)
    keyval = dot(weight[local:, :], normed, NT)
    key = rotated(keyval[:local] + column(qcol, owner, local, 1), cos, sin, hdim)
    value = (keyval[local:] + column(qcol, owner, local, 2)).astype(jnp.bfloat16)
    qout[...] = query
    kout[...] = key
    vout[...] = value
    for p in range(local // (2 * hdim)):
        f = slice(2 * p * hdim, 2 * (p + 1) * hdim)
        scores = dot(key[f], query[f], TN)
        top = jnp.max(scores, axis=0, keepdims=True)
        expo = jnp.exp2((scores - top) * scale)
        tops[p : p + 1, :] = top
        sums[p : p + 1, :] = jnp.sum(expo, axis=0, keepdims=True)
        total = dot(value[f], expo.astype(jnp.bfloat16), NN)
        outs[f.start : f.start + hdim, :] = total[:hdim, :rows]
        outs[f.start + hdim : f.stop, :] = total[hdim:, rows:]
    if side:
        copy.wait()


def far_kernel(hdim, xa, xb, wown, wpair, pall, qcol, cosine, sine, *refs):
    scale = math.log2(math.e) / math.sqrt(hdim)
    near, (part, send, kout, vout, raw, expos, attended) = (refs[:4], refs[4:8]), refs[8:]
    local = wown.shape[0] // 3
    rows = xa.shape[0]
    me = lax.axis_index("sp")
    normed = jnp.concatenate([xa[...], xb[...]], axis=0)
    cos, sin = cosine[:, 2 * rows :], sine[:, 2 * rows :]
    pairs = local // (2 * hdim)
    tops, shrinks, invs = {}, {}, {}

    def place(side, p):
        f = slice(2 * p * hdim, 2 * (p + 1) * hdim)
        return f, slice(side * local + f.start, side * local + f.stop)

    def project(side, c):
        weight = (wown, wpair)[side][c * local : (c + 1) * local, :]
        return dot(weight, normed, NT) + column(qcol, me ^ side, local, c)

    for side in range(2):
        kout[side * local : (side + 1) * local, :] = rotated(project(side, 1), cos, sin, hdim)
    for side in range(2):
        for p in range(pairs):
            f, g = place(side, p)
            scores = dot(kout[g, :], near[side][0][f, :], TN)
            raw[side * pairs + p] = scores
            old = near[side][1][p : p + 1, :]
            tops[side, p] = jnp.maximum(old, jnp.max(scores, axis=0, keepdims=True))
    for side in range(2):
        vout[side * local : (side + 1) * local, :] = project(side, 2).astype(jnp.bfloat16)
        for p in range(pairs):
            top = tops[side, p]
            expo = jnp.exp2((raw[side * pairs + p] - top) * scale)
            expos[side * pairs + p] = expo.astype(jnp.bfloat16)
            shrink = jnp.exp2((near[side][1][p : p + 1, :] - top) * scale)
            shrinks[side, p] = shrink
            sums = near[side][2][p : p + 1, :]
            invs[side, p] = 1.0 / (sums * shrink + jnp.sum(expo, axis=0, keepdims=True))
    for side in range(2):
        for p in range(pairs):
            f, g = place(side, p)
            late = dot(vout[g, :], expos[side * pairs + p], NN)
            for h in range(2):
                lanes = slice(h * rows, (h + 1) * rows)
                feats = slice(h * hdim, (h + 1) * hdim)
                early = near[side][3][f.start + h * hdim : f.start + (h + 1) * hdim, :]
                mixed = (early * shrinks[side, p][:, lanes] + late[feats, lanes]) * invs[side, p][:, lanes]
                attended[g.start + h * hdim : g.start + (h + 1) * hdim, :] = mixed.astype(jnp.bfloat16)
    total = dot(attended[...], pall[...], TN)
    part[...] = total
    send[...] = total.astype(jnp.bfloat16)


def late_kernel(hdim, x, wown, wpair, pall, qcol, cosine, sine, kna, vna, knb, vnb, kf, vf, part, send0, send1):
    scale = math.log2(math.e) / math.sqrt(hdim)
    local = wown.shape[0] // 3
    rows = x.shape[0]
    me = lax.axis_index("sp")
    pieces = []
    for side, weight in enumerate((wown, wpair)):
        query = dot(weight[:local, :], x[...], NT) + column(qcol, me ^ side, local, 0)
        far = slice(2 * rows, 3 * rows)
        query = paired(rotated(query, cosine[:, far], sine[:, far], hdim), hdim)
        for at in range(0, local, 2 * hdim):
            f = slice(side * local + at, side * local + at + 2 * hdim)
            g = slice(at, at + 2 * hdim)
            kn, vn = ((kna, vna), (knb, vnb))[side]
            both = query[g]
            sn = dot(kn[g, :], both, TN)
            sf = dot(kf[f, :], both, TN)
            top = jnp.maximum(jnp.max(sn, axis=0, keepdims=True), jnp.max(sf, axis=0, keepdims=True))
            en = jnp.exp2((sn - top) * scale)
            ef = jnp.exp2((sf - top) * scale)
            inv = 1.0 / (jnp.sum(en, axis=0, keepdims=True) + jnp.sum(ef, axis=0, keepdims=True))
            mixed = dot(vn[g, :], (en * inv).astype(jnp.bfloat16), NN)
            mixed = (mixed + dot(vf[f, :], (ef * inv).astype(jnp.bfloat16), NN)).astype(jnp.bfloat16)
            pieces += [mixed[:hdim, :rows], mixed[hdim:, rows:]]
    total = dot(jnp.concatenate(pieces, axis=0), pall[...], TN)
    part[...] = total
    cut = send0.shape[0]
    send0[...] = total[:cut].astype(jnp.bfloat16)
    send1[...] = total[cut:].astype(jnp.bfloat16)


def merge_kernel(keep, start, x, part, got, rows, *rest):
    blocks, scratch = rest[-2], rest[-1]
    width = x.shape[1]
    place = slice(start, start + got.shape[0])
    value = x[place, :].astype(jnp.float32) + (part[place, :] + got[...].astype(jnp.float32)) + rows[2:3, :]
    rounded = value.astype(jnp.bfloat16)
    if keep:
        rest[-3][...] = rounded
    normed = layer_norm(rounded.astype(jnp.float32), rows[3:4, :], rows[4:5, :])
    count = got.shape[0] // 4
    lanes = scratch.shape[2]
    for t in range(width // lanes):
        scratch[t] = normed[:, t * lanes : (t + 1) * lanes]
        for j in range(4):
            at = j * width + t * lanes
            blocks[:, at : at + lanes] = scratch[t, pl.ds(j, count, stride=4), :].astype(jnp.bfloat16)


def gelu(v):
    return 0.5 * v * (1.0 + lax.erf(v * math.sqrt(0.5)))


def hidden_kernel(own, pair, weight, rows, out):
    core = lax.axis_index("sp") % 2
    count = own.shape[0]
    both = jnp.concatenate([own[...], pair[...]] * 2, axis=0)
    hid = gelu(dot(both, weight[...], NN)[: 2 * count] + rows[5:6, :]).astype(jnp.bfloat16)
    for half, place in enumerate((core, 1 - core)):
        out[pl.ds(pl.multiple_of(place * count, count), count), :] = hid[half * count : (half + 1) * count]


def last_kernel(own0, own1, pair0, pair1, weight, rows, vit0, vit1, early, out, vout, stage, sems):
    me = lax.axis_index("sp")
    chip, core = me // 2, me % 2
    count = own0.shape[0] + own1.shape[0]
    cut, rest = vit0.shape[0], vit1.shape[0]
    at = lambda start: pl.ds(pl.multiple_of(start, count), count)
    there = out.at[pl.ds(pl.multiple_of((1 - chip) * 2 * count, count), 2 * count)]
    copies = [
        pltpu.make_async_copy(vit0, vout.at[pl.ds(0, cut)], sems.at[0]),
        pltpu.make_async_copy(vit1, vout.at[pl.ds(cut, rest)], sems.at[1]),
        pltpu.make_async_copy(early, there, sems.at[2]),
    ]
    for copy in copies:
        copy.start()
    both = jnp.concatenate([x[...] for x in (own0, own1, pair0, pair1)] * 2, axis=0)
    step = stage.shape[2]
    for n in range(stage.shape[0]):
        cols = slice(n * step, (n + 1) * step)
        value = dot(both, weight[:, cols], NN)[: 2 * count] + rows[5:6, cols]
        stage[n] = gelu(value).astype(jnp.bfloat16)
        for side, place in enumerate((core, 1 - core)):
            copy = pltpu.make_async_copy(
                stage.at[n, pl.ds(side * count, count)],
                out.at[at(chip * 2 * count + place * count), pl.ds(n * step, step)],
                sems.at[3 + 2 * n + side],
            )
            copy.start()
            copies.append(copy)
    for copy in copies:
        copy.wait()


def shape(dims, dtype=jnp.bfloat16):
    return jax.ShapeDtypeStruct(dims, dtype)


def two_chips(
    patches,
    pos_ids,
    norm_gain,
    norm_bias,
    qkv_weight,
    qkv_bias,
    proj_weight,
    proj_bias,
    merge_gain,
    merge_bias,
    fc1_weight,
    fc1_bias,
):
    prow, width = patches.shape
    hdim = width // HEADS
    local = qkv_weight.shape[2]
    hidden = fc1_weight.shape[1]

    def swap(value, bit):
        return lax.ppermute(value, "sp", [(i, i ^ bit) for i in range(4)])

    weight = qkv_weight.transpose(1, 2, 0).reshape(3 * local, width)
    x_far = swap(patches, 2)
    x_pair = swap(patches, 1)
    w_pair = swap(weight, 1)
    p_pair = swap(proj_weight, 1)

    both = 2 * local
    mul = 2 * prow * width * local * 2
    table = shape((hdim // 2, 4 * prow), jnp.float32)

    sources = (patches, pos_ids, qkv_bias, norm_gain, norm_bias, proj_bias, merge_gain, merge_bias, fc1_bias)
    sources += (proj_weight, weight)
    held = lambda v: pltpu.VMEM(v.shape, v.dtype)
    x_own, w_own, p_half, n_own, rows, qcol, cos, sin = pl.pallas_call(
        functools.partial(setup_kernel, hdim, len(sources)),
        out_shape=(
            held(patches),
            held(weight),
            pltpu.VMEM((both, width), proj_weight.dtype),
            shape((prow, width)),
            shape((8, width), jnp.float32),
            shape((width, 8), jnp.float32),
            table,
            table,
        ),
        in_specs=[HBM] * len(sources),
        scratch_shapes=[held(v) for v in sources[1:-2]] + [pltpu.SemaphoreType.DMA((len(sources),))],
        compiler_params=pltpu.CompilerParams(vmem_limit_bytes=4 * MIB),
        cost_estimate=pl.CostEstimate(flops=mul, bytes_accessed=1 << 22, transcendentals=0),
        name="setup",
    )(*(pltpu.with_memory_space_constraint(v, pltpu.HBM) for v in sources))

    def norm(x, start, count, *after):
        return pl.pallas_call(
            functools.partial(norm_kernel, start),
            out_shape=shape((count, width)),
            in_specs=[VMEM] * 2 + [ANY] * len(after),
            compiler_params=pltpu.CompilerParams(vmem_limit_bytes=4 * MIB),
            cost_estimate=pl.CostEstimate(flops=mul // 4, bytes_accessed=1 << 20, transcendentals=0),
        )(x, rows, *after)

    n_pair = norm(x_pair, 0, prow)
    flat = shape((local, 2 * prow))
    state = shape((local // (2 * hdim), 2 * prow), jnp.float32)
    near_shape = (flat, flat, flat, state, state, shape((local, prow), jnp.float32))

    def near(side, weight, *more):
        return pl.pallas_call(
            functools.partial(near_kernel, hdim, side),
            out_shape=near_shape + (pltpu.VMEM((both, width), proj_weight.dtype),) * side,
            input_output_aliases={7: 6} if side else {},
            scratch_shapes=[pltpu.SemaphoreType.DMA] * side,
            compiler_params=pltpu.CompilerParams(vmem_limit_bytes=8 * MIB),
            cost_estimate=pl.CostEstimate(flops=4 * mul, bytes_accessed=1 << 22, transcendentals=0),
        )(n_own, n_pair, weight, qcol, cos, sin, *more)

    q, *kv_own, tops, sums, outs = near(0, w_own)
    early_own = (q, tops, sums, outs)
    q, *kv_pair, tops, sums, outs, p_all = near(1, w_pair, p_pair, p_half)
    early_pair = (q, tops, sums, outs)

    n_far = norm(x_far, 0, prow, early_own[1], p_all)
    n_farpair = swap(n_far, 1)
    tall = shape((both, 2 * prow))
    shared = (w_own, w_pair, p_all, qcol, cos, sin)
    part_shape = shape((prow, width), jnp.float32)
    folds = both // (2 * hdim)
    part0, send0, k_far, v_far = pl.pallas_call(
        functools.partial(far_kernel, hdim),
        out_shape=(part_shape, shape((prow, width)), tall, tall),
        scratch_shapes=[
            pltpu.VMEM((folds, 2 * prow, 2 * prow), jnp.float32),
            pltpu.VMEM((folds, 2 * prow, 2 * prow), jnp.bfloat16),
            pltpu.VMEM((both, prow), jnp.bfloat16),
        ],
        compiler_params=pltpu.CompilerParams(vmem_limit_bytes=8 * MIB),
        cost_estimate=pl.CostEstimate(flops=6 * mul, bytes_accessed=1 << 22, transcendentals=0),
        name="far",
    )(n_far, n_farpair, *shared, *early_own, *early_pair)
    got1 = swap(send0, 2)
    cut = prow * 3 // 4
    halves = (shape((cut, width)), shape((prow - cut, width)))
    part1, send1a, send1b = call(
        functools.partial(late_kernel, hdim), (part_shape,) + halves, 8 * MIB, 6 * mul
    )(n_far, *shared, *kv_own, *kv_pair, k_far, v_far)
    got0a = swap(send1a, 2)
    got0b = swap(send1b, 2)
    late_rows = call(copy_kernel, shape(rows.shape, rows.dtype), MIB, 1000)(rows)

    def merge(keep, start, x, part, got, late_rows, *after):
        count = got.shape[0]
        outs = (shape((count, width)),) * keep + (shape((count // 4, 4 * width)),)
        return pl.pallas_call(
            functools.partial(merge_kernel, keep, start),
            out_shape=outs,
            in_specs=[VMEM] * 4 + [ANY] * len(after),
            scratch_shapes=[pltpu.VMEM((width // 128, count, 128), jnp.float32)],
            compiler_params=pltpu.CompilerParams(vmem_limit_bytes=4 * MIB),
            cost_estimate=pl.CostEstimate(flops=mul // 4, bytes_accessed=1 << 20, transcendentals=0),
        )(x, part, got, late_rows, *after)

    fc1 = pltpu.with_memory_space_constraint(fc1_weight, pltpu.VMEM)
    (blocks1,) = merge(0, 0, x_far, part1, got1, late_rows)
    pair1 = swap(blocks1, 1)
    flops = prow * 4 * width * hidden
    early = call(hidden_kernel, shape((prow // 2, hidden)), 4 * MIB, flops)(blocks1, pair1, fc1, rows)
    vit_a, blocks_a = merge(1, 0, x_own, part0, got0a, late_rows, early)
    pair_a = swap(blocks_a, 1)
    late_rows = call(copy_kernel, shape(rows.shape, rows.dtype), MIB, 1000)(late_rows)
    vit_b, blocks_b = merge(1, cut, x_own, part0, got0b, late_rows)
    pair_b = swap(blocks_b, 1)
    parts = hidden // 256
    merged, vit_out = pl.pallas_call(
        last_kernel,
        out_shape=(shape((prow, hidden)), shape((prow, width))),
        out_specs=[HBM] * 2,
        scratch_shapes=[
            pltpu.VMEM((parts, prow // 2, 256), jnp.bfloat16),
            pltpu.SemaphoreType.DMA((3 + 2 * parts,)),
        ],
        compiler_params=pltpu.CompilerParams(vmem_limit_bytes=4 * MIB),
        cost_estimate=pl.CostEstimate(flops=flops, bytes_accessed=1 << 24, transcendentals=0),
        name="hidden0",
    )(blocks_a, blocks_b, pair_a, pair_b, fc1, rows, vit_a, vit_b, early)
    return vit_out, merged


def rotate(values, positions, nheads):
    count = values.shape[0]
    hdim = values.shape[1] // nheads
    quarter = hdim // 4
    inv = 1.0 / 10000.0 ** (jnp.arange(quarter, dtype=jnp.float32) * 2.0 / (hdim // 2))
    rows = positions[0].astype(jnp.float32)[:, None] * inv
    cols = positions[1].astype(jnp.float32)[:, None] * inv
    angle = jnp.concatenate([rows, cols, rows, cols], axis=1)
    cosine = jnp.cos(angle)[:, None, :]
    sine = jnp.sin(angle)[:, None, :]
    shaped = values.reshape(count, nheads, hdim)
    half = hdim // 2
    turned = jnp.concatenate([-shaped[..., half:], shaped[..., :half]], axis=-1)
    return (shaped * cosine + turned * sine).reshape(count, nheads * hdim)


def attend_blocks(query, keys, value, nheads, hdim):
    count = query.shape[0]
    block = min(512, count)
    qblocks = query.reshape(count // block, block, nheads, hdim)
    kshaped = keys.reshape(count, nheads, hdim)
    vshaped = value.reshape(count, nheads, hdim)
    scale = 1.0 / jnp.sqrt(jnp.float32(hdim))

    def one_block(qpart):
        scores = jnp.einsum("bhd,khd->hbk", qpart, kshaped, preferred_element_type=jnp.float32) * scale
        top = jnp.max(scores, axis=-1, keepdims=True)
        expo = jnp.exp(scores - top)
        weights = (expo / jnp.sum(expo, axis=-1, keepdims=True)).astype(jnp.bfloat16)
        result = jnp.einsum("hbk,khd->bhd", weights, vshaped, preferred_element_type=jnp.float32)
        return result.astype(jnp.bfloat16).reshape(block, nheads * hdim)

    return lax.map(one_block, qblocks).reshape(count, nheads * hdim)


def any_size(
    patches,
    pos_ids,
    norm_gain,
    norm_bias,
    qkv_weight,
    qkv_bias,
    proj_weight,
    proj_bias,
    merge_gain,
    merge_bias,
    fc1_weight,
    fc1_bias,
):
    groups = lax.axis_size("sp")
    where = lax.axis_index("sp")
    prow, width = patches.shape
    heads_local = HEADS // groups
    hdim = width // HEADS
    local_width = width // groups
    xfloat = patches.astype(jnp.float32)
    normed = layer_norm(xfloat, norm_gain, norm_bias).astype(jnp.bfloat16)
    bias_local = lax.dynamic_slice_in_dim(qkv_bias, where * local_width, local_width, 1)
    qkv = (
        jnp.einsum(
            "pd,dcn->pcn",
            lax.all_gather(normed, "sp", axis=0, tiled=True),
            qkv_weight,
            preferred_element_type=jnp.float32,
        )
        + bias_local[None]
    )
    query = rotate(qkv[:, 0], pos_ids, heads_local).astype(jnp.bfloat16)
    keys = rotate(qkv[:, 1], pos_ids, heads_local).astype(jnp.bfloat16)
    value = qkv[:, 2].astype(jnp.bfloat16)
    attended = attend_blocks(query, keys, value, heads_local, hdim)
    returned = lax.all_to_all(attended, "sp", split_axis=0, concat_axis=1, tiled=True)
    projected = jnp.dot(
        returned,
        lax.all_gather(proj_weight, "sp", axis=0, tiled=True),
        preferred_element_type=jnp.float32,
    )
    vit_out = (xfloat + projected + proj_bias).astype(jnp.bfloat16)
    zn = layer_norm(vit_out.astype(jnp.float32), merge_gain, merge_bias).astype(jnp.bfloat16)
    blocks = zn.reshape(prow // 4, 4 * width)
    hidden = (
        jnp.dot(
            lax.all_gather(blocks, "sp", axis=0, tiled=True),
            fc1_weight,
            preferred_element_type=jnp.float32,
        )
        + fc1_bias
    )
    merged_hidden = jax.nn.gelu(hidden, approximate=False).astype(jnp.bfloat16)
    return (vit_out, merged_hidden)


def per_device(*args):
    if lax.axis_size("sp") == 4:
        return two_chips(*args)
    return any_size(*args)


def solution(mesh):
    return jax.shard_map(
        per_device,
        mesh=mesh,
        in_specs=(
            P(("img", "sp"), None),
            P(None, "img"),
            P(),
            P(),
            P(None, None, "sp"),
            P(),
            P("sp", None),
            P(),
            P(),
            P(),
            P(None, "sp"),
            P("sp"),
        ),
        out_specs=(P(("img", "sp"), None), P("img", "sp")),
        check_vma=False,
    )
```

```python
import functools
import math

import jax
import jax.numpy as jnp
from jax import lax
from jax.experimental import pallas as pl
from jax.experimental.pallas import tpu as pltpu
from jax.sharding import PartitionSpec as P


HEADS = 16
EPS = 1e-06
MIB = 1 << 20
VMEM = pl.BlockSpec(memory_space=pltpu.VMEM)
ANY = pl.BlockSpec(memory_space=pl.ANY)
HBM = pl.BlockSpec(memory_space=pltpu.HBM)
NT = (((1,), (1,)), ((), ()))
TN = (((0,), (0,)), ((), ()))
NN = (((1,), (0,)), ((), ()))


def layer_norm(values, gain, bias):
    mean = jnp.mean(values, axis=-1, keepdims=True)
    centered = values - mean
    var = jnp.mean(centered * centered, axis=-1, keepdims=True)
    return centered * lax.rsqrt(var + EPS) * gain + bias


def dot(a, b, dims):
    return lax.dot_general(a, b, dims, preferred_element_type=jnp.float32)


def call(kernel, outs, nbytes, flops):
    return pl.pallas_call(
        kernel,
        out_shape=outs,
        compiler_params=pltpu.CompilerParams(vmem_limit_bytes=nbytes),
        cost_estimate=pl.CostEstimate(flops=flops, bytes_accessed=1 << 20, transcendentals=0),
    )


def setup_kernel(hdim, count, *refs):
    sources, rest = refs[:count], refs[count:]
    x, wown, pall, normed, rows, qcol, cosine, sine, pos, qkv_bias = rest[:10]
    vectors, sems = rest[10:-1], rest[-1]
    targets = (x, pos, qkv_bias) + tuple(vectors) + (pall.at[pl.ds(0, pall.shape[0] // 2)], wown)
    copies = [pltpu.make_async_copy(a, b, sems.at[n]) for n, (a, b) in enumerate(zip(sources, targets))]
    for copy in copies:
        copy.start()
    prow, width = x.shape
    me = lax.axis_index("sp")
    quarter = hdim // 4
    feature = lax.broadcasted_iota(jnp.int32, (2 * quarter, prow), 0)
    second = feature >= quarter
    power = jnp.where(second, feature - quarter, feature).astype(jnp.float32)
    inv = jnp.exp(power * (-2.0 * math.log(10000.0) / (hdim // 2)))
    rows[...] = jnp.zeros_like(rows)
    for copy in copies[:-2]:
        copy.wait()
    for k in range(4):
        at = pl.ds(pl.multiple_of((me ^ k) * prow, prow), prow)
        place = jnp.where(second, pos[1:2, at], pos[0:1, at]).astype(jnp.float32)
        angle = place * inv
        cosine[:, k * prow : (k + 1) * prow] = jnp.cos(angle)
        sine[:, k * prow : (k + 1) * prow] = jnp.sin(angle)
    for at, vector in enumerate(vectors):
        rows[at : at + 1, :] = vector[...].reshape(1, width)
    cube = jnp.concatenate([qkv_bias[...], jnp.zeros((5, width), jnp.float32)], axis=0)
    qcol[...] = cube.T
    value = layer_norm(x[...].astype(jnp.float32), rows[0:1, :], rows[1:2, :])
    normed[...] = value.astype(jnp.bfloat16)
    for copy in copies[-2:]:
        copy.wait()


def copy_kernel(x, out):
    out[...] = x[...]


def norm_kernel(start, x, rows, *rest):
    out = rest[-1]
    value = x[start : start + out.shape[0], :].astype(jnp.float32)
    out[...] = layer_norm(value, rows[0:1, :], rows[1:2, :]).astype(jnp.bfloat16)


def column(qcol, owner, local, c):
    return qcol[pl.ds(pl.multiple_of(owner * local, 8), local), c : c + 1]


def rotated(raw, cos, sin, hdim):
    half = hdim // 2
    pieces = []
    for at in range(0, raw.shape[0], hdim):
        top, low = raw[at : at + half], raw[at + half : at + hdim]
        pieces += [top * cos - low * sin, low * cos + top * sin]
    return jnp.concatenate(pieces, axis=0).astype(jnp.bfloat16)


def paired(query, hdim):
    zero = jnp.zeros((hdim, query.shape[1]), query.dtype)
    rows = []
    for at in range(0, query.shape[0], 2 * hdim):
        rows.append(jnp.concatenate([query[at : at + hdim], zero], axis=1))
        rows.append(jnp.concatenate([zero, query[at + hdim : at + 2 * hdim]], axis=1))
    return jnp.concatenate(rows, axis=0)


def near_kernel(hdim, side, xa, xb, weight, qcol, cosine, sine, *rest):
    qout, kout, vout, tops, sums, outs = rest
    scale = math.log2(math.e) / math.sqrt(hdim)
    local = weight.shape[0] // 3
    rows = xa.shape[0]
    owner = lax.axis_index("sp") ^ side
    normed = jnp.concatenate([xa[...], xb[...]], axis=0)
    cos, sin = cosine[:, : 2 * rows], sine[:, : 2 * rows]
    query = dot(weight[0:local, :], normed[:rows], NT) + column(qcol, owner, local, 0)
    query = paired(rotated(query, cos[:, :rows], sin[:, :rows], hdim), hdim)
    keyval = dot(weight[local:, :], normed, NT)
    key = rotated(keyval[:local] + column(qcol, owner, local, 1), cos, sin, hdim)
    value = (keyval[local:] + column(qcol, owner, local, 2)).astype(jnp.bfloat16)
    qout[...] = query
    kout[...] = key
    vout[...] = value
    for p in range(local // (2 * hdim)):
        f = slice(2 * p * hdim, 2 * (p + 1) * hdim)
        scores = dot(key[f], query[f], TN)
        top = jnp.max(scores, axis=0, keepdims=True)
        expo = jnp.exp2((scores - top) * scale)
        tops[p : p + 1, :] = top
        sums[p : p + 1, :] = jnp.sum(expo, axis=0, keepdims=True)
        total = dot(value[f], expo.astype(jnp.bfloat16), NN)
        outs[f.start : f.start + hdim, :] = total[:hdim, :rows]
        outs[f.start + hdim : f.stop, :] = total[hdim:, rows:]


def gather_kernel(ppair, half, after, pall, sem):
    del half, after
    count = ppair.shape[0]
    copy = pltpu.make_async_copy(ppair, pall.at[pl.ds(count, count)], sem)
    copy.start()
    copy.wait()


def far_kernel(hdim, xa, xb, wown, wpair, pall, qcol, cosine, sine, *refs):
    scale = math.log2(math.e) / math.sqrt(hdim)
    near, (part, send, kout, vout, raw, expos, attended) = (refs[:4], refs[4:8]), refs[8:]
    local = wown.shape[0] // 3
    rows = xa.shape[0]
    me = lax.axis_index("sp")
    normed = jnp.concatenate([xa[...], xb[...]], axis=0)
    cos, sin = cosine[:, 2 * rows :], sine[:, 2 * rows :]
    pairs = local // (2 * hdim)
    tops, shrinks, invs = {}, {}, {}

    def place(side, p):
        f = slice(2 * p * hdim, 2 * (p + 1) * hdim)
        return f, slice(side * local + f.start, side * local + f.stop)

    def project(side, c):
        weight = (wown, wpair)[side][c * local : (c + 1) * local, :]
        return dot(weight, normed, NT) + column(qcol, me ^ side, local, c)

    for side in range(2):
        kout[side * local : (side + 1) * local, :] = rotated(project(side, 1), cos, sin, hdim)
    for side in range(2):
        vout[side * local : (side + 1) * local, :] = project(side, 2).astype(jnp.bfloat16)
    for side in range(2):
        for p in range(pairs):
            f, g = place(side, p)
            scores = dot(kout[g, :], near[side][0][f, :], TN)
            raw[side * pairs + p] = scores
            old = near[side][1][p : p + 1, :]
            tops[side, p] = jnp.maximum(old, jnp.max(scores, axis=0, keepdims=True))
    for side in range(2):
        for p in range(pairs):
            top = tops[side, p]
            expo = jnp.exp2((raw[side * pairs + p] - top) * scale)
            expos[side * pairs + p] = expo.astype(jnp.bfloat16)
            shrink = jnp.exp2((near[side][1][p : p + 1, :] - top) * scale)
            shrinks[side, p] = shrink
            sums = near[side][2][p : p + 1, :]
            invs[side, p] = 1.0 / (sums * shrink + jnp.sum(expo, axis=0, keepdims=True))
    for side in range(2):
        for p in range(pairs):
            f, g = place(side, p)
            late = dot(vout[g, :], expos[side * pairs + p], NN)
            for h in range(2):
                lanes = slice(h * rows, (h + 1) * rows)
                feats = slice(h * hdim, (h + 1) * hdim)
                early = near[side][3][f.start + h * hdim : f.start + (h + 1) * hdim, :]
                mixed = (early * shrinks[side, p][:, lanes] + late[feats, lanes]) * invs[side, p][:, lanes]
                attended[g.start + h * hdim : g.start + (h + 1) * hdim, :] = mixed.astype(jnp.bfloat16)
    total = dot(attended[...], pall[...], TN)
    part[...] = total
    send[...] = total.astype(jnp.bfloat16)


def late_kernel(hdim, x, wown, wpair, pall, qcol, cosine, sine, kna, vna, knb, vnb, kf, vf, part, send0, send1):
    scale = math.log2(math.e) / math.sqrt(hdim)
    local = wown.shape[0] // 3
    rows = x.shape[0]
    me = lax.axis_index("sp")
    pieces = []
    for side, weight in enumerate((wown, wpair)):
        query = dot(weight[:local, :], x[...], NT) + column(qcol, me ^ side, local, 0)
        far = slice(2 * rows, 3 * rows)
        query = paired(rotated(query, cosine[:, far], sine[:, far], hdim), hdim)
        for at in range(0, local, 2 * hdim):
            f = slice(side * local + at, side * local + at + 2 * hdim)
            g = slice(at, at + 2 * hdim)
            kn, vn = ((kna, vna), (knb, vnb))[side]
            both = query[g]
            sn = dot(kn[g, :], both, TN)
            sf = dot(kf[f, :], both, TN)
            top = jnp.maximum(jnp.max(sn, axis=0, keepdims=True), jnp.max(sf, axis=0, keepdims=True))
            en = jnp.exp2((sn - top) * scale)
            ef = jnp.exp2((sf - top) * scale)
            inv = 1.0 / (jnp.sum(en, axis=0, keepdims=True) + jnp.sum(ef, axis=0, keepdims=True))
            mixed = dot(vn[g, :], (en * inv).astype(jnp.bfloat16), NN)
            mixed = (mixed + dot(vf[f, :], (ef * inv).astype(jnp.bfloat16), NN)).astype(jnp.bfloat16)
            pieces += [mixed[:hdim, :rows], mixed[hdim:, rows:]]
    total = dot(jnp.concatenate(pieces, axis=0), pall[...], TN)
    part[...] = total
    cut = send0.shape[0]
    send0[...] = total[:cut].astype(jnp.bfloat16)
    send1[...] = total[cut:].astype(jnp.bfloat16)


def merge_kernel(keep, start, x, part, got, rows, *rest):
    blocks, scratch = rest[-2], rest[-1]
    width = x.shape[1]
    place = slice(start, start + got.shape[0])
    value = x[place, :].astype(jnp.float32) + (part[place, :] + got[...].astype(jnp.float32)) + rows[2:3, :]
    rounded = value.astype(jnp.bfloat16)
    if keep:
        rest[-3][...] = rounded
    normed = layer_norm(rounded.astype(jnp.float32), rows[3:4, :], rows[4:5, :])
    count = got.shape[0] // 4
    lanes = scratch.shape[2]
    for t in range(width // lanes):
        scratch[t] = normed[:, t * lanes : (t + 1) * lanes]
        for j in range(4):
            at = j * width + t * lanes
            blocks[:, at : at + lanes] = scratch[t, pl.ds(j, count, stride=4), :].astype(jnp.bfloat16)


def gelu(v):
    return 0.5 * v * (1.0 + lax.erf(v * math.sqrt(0.5)))


def hidden_kernel(own, pair, weight, rows, out):
    core = lax.axis_index("sp") % 2
    count = own.shape[0]
    both = jnp.concatenate([own[...], pair[...]] * 2, axis=0)
    hid = gelu(dot(both, weight[...], NN)[: 2 * count] + rows[5:6, :]).astype(jnp.bfloat16)
    for half, place in enumerate((core, 1 - core)):
        out[pl.ds(pl.multiple_of(place * count, count), count), :] = hid[half * count : (half + 1) * count]


def last_kernel(own0, own1, pair0, pair1, weight, rows, vit0, vit1, early, out, vout, stage, sems):
    me = lax.axis_index("sp")
    chip, core = me // 2, me % 2
    count = own0.shape[0] + own1.shape[0]
    cut, rest = vit0.shape[0], vit1.shape[0]
    at = lambda start: pl.ds(pl.multiple_of(start, count), count)
    there = out.at[pl.ds(pl.multiple_of((1 - chip) * 2 * count, count), 2 * count)]
    copies = [
        pltpu.make_async_copy(vit0, vout.at[pl.ds(0, cut)], sems.at[0]),
        pltpu.make_async_copy(vit1, vout.at[pl.ds(cut, rest)], sems.at[1]),
        pltpu.make_async_copy(early, there, sems.at[2]),
    ]
    for copy in copies:
        copy.start()
    both = jnp.concatenate([x[...] for x in (own0, own1, pair0, pair1)] * 2, axis=0)
    step = stage.shape[2]
    for n in range(stage.shape[0]):
        cols = slice(n * step, (n + 1) * step)
        value = dot(both, weight[:, cols], NN)[: 2 * count] + rows[5:6, cols]
        stage[n] = gelu(value).astype(jnp.bfloat16)
        for side, place in enumerate((core, 1 - core)):
            copy = pltpu.make_async_copy(
                stage.at[n, pl.ds(side * count, count)],
                out.at[at(chip * 2 * count + place * count), pl.ds(n * step, step)],
                sems.at[3 + 2 * n + side],
            )
            copy.start()
            copies.append(copy)
    for copy in copies:
        copy.wait()


def shape(dims, dtype=jnp.bfloat16):
    return jax.ShapeDtypeStruct(dims, dtype)


def two_chips(
    patches,
    pos_ids,
    norm_gain,
    norm_bias,
    qkv_weight,
    qkv_bias,
    proj_weight,
    proj_bias,
    merge_gain,
    merge_bias,
    fc1_weight,
    fc1_bias,
):
    prow, width = patches.shape
    hdim = width // HEADS
    local = qkv_weight.shape[2]
    hidden = fc1_weight.shape[1]

    def swap(value, bit):
        return lax.ppermute(value, "sp", [(i, i ^ bit) for i in range(4)])

    weight = qkv_weight.transpose(1, 2, 0).reshape(3 * local, width)
    x_far = swap(patches, 2)
    x_pair = swap(patches, 1)
    w_pair = swap(weight, 1)
    p_pair = swap(proj_weight, 1)

    both = 2 * local
    mul = 2 * prow * width * local * 2
    table = shape((hdim // 2, 4 * prow), jnp.float32)

    sources = (patches, pos_ids, qkv_bias, norm_gain, norm_bias, proj_bias, merge_gain, merge_bias, fc1_bias)
    sources += (proj_weight, weight)
    held = lambda v: pltpu.VMEM(v.shape, v.dtype)
    x_own, w_own, p_half, n_own, rows, qcol, cos, sin = pl.pallas_call(
        functools.partial(setup_kernel, hdim, len(sources)),
        out_shape=(
            held(patches),
            held(weight),
            pltpu.VMEM((both, width), proj_weight.dtype),
            shape((prow, width)),
            shape((8, width), jnp.float32),
            shape((width, 8), jnp.float32),
            table,
            table,
        ),
        in_specs=[HBM] * len(sources),
        scratch_shapes=[held(v) for v in sources[1:-2]] + [pltpu.SemaphoreType.DMA((len(sources),))],
        compiler_params=pltpu.CompilerParams(vmem_limit_bytes=4 * MIB),
        cost_estimate=pl.CostEstimate(flops=mul, bytes_accessed=1 << 22, transcendentals=0),
        name="setup",
    )(*(pltpu.with_memory_space_constraint(v, pltpu.HBM) for v in sources))

    def norm(x, start, count, *after):
        return pl.pallas_call(
            functools.partial(norm_kernel, start),
            out_shape=shape((count, width)),
            in_specs=[VMEM] * 2 + [ANY] * len(after),
            compiler_params=pltpu.CompilerParams(vmem_limit_bytes=4 * MIB),
            cost_estimate=pl.CostEstimate(flops=mul // 4, bytes_accessed=1 << 20, transcendentals=0),
        )(x, rows, *after)

    n_pair = norm(x_pair, 0, prow)
    flat = shape((local, 2 * prow))
    state = shape((local // (2 * hdim), 2 * prow), jnp.float32)
    near_shape = (flat, flat, flat, state, state, shape((local, prow), jnp.float32))

    def near(side, weight):
        return call(
            functools.partial(near_kernel, hdim, side), near_shape, 8 * MIB, 4 * mul
        )(n_own, n_pair, weight, qcol, cos, sin)

    q, *kv_own, tops, sums, outs = near(0, w_own)
    early_own = (q, tops, sums, outs)
    q, *kv_pair, tops, sums, outs = near(1, w_pair)
    early_pair = (q, tops, sums, outs)

    n_far = norm(x_far, 0, prow, early_own[1], early_pair[1])
    n_farpair = swap(n_far, 1)
    p_all = pl.pallas_call(
        gather_kernel,
        out_shape=pltpu.VMEM((both, width), proj_weight.dtype),
        in_specs=[VMEM, VMEM, ANY],
        input_output_aliases={1: 0},
        scratch_shapes=[pltpu.SemaphoreType.DMA],
        compiler_params=pltpu.CompilerParams(vmem_limit_bytes=2 * MIB),
        cost_estimate=pl.CostEstimate(flops=mul // 4, bytes_accessed=1 << 20, transcendentals=0),
        name="gather_proj",
    )(p_pair, p_half, n_far)
    tall = shape((both, 2 * prow))
    shared = (w_own, w_pair, p_all, qcol, cos, sin)
    part_shape = shape((prow, width), jnp.float32)
    folds = both // (2 * hdim)
    part0, send0, k_far, v_far = pl.pallas_call(
        functools.partial(far_kernel, hdim),
        out_shape=(part_shape, shape((prow, width)), tall, tall),
        scratch_shapes=[
            pltpu.VMEM((folds, 2 * prow, 2 * prow), jnp.float32),
            pltpu.VMEM((folds, 2 * prow, 2 * prow), jnp.bfloat16),
            pltpu.VMEM((both, prow), jnp.bfloat16),
        ],
        compiler_params=pltpu.CompilerParams(vmem_limit_bytes=8 * MIB),
        cost_estimate=pl.CostEstimate(flops=6 * mul, bytes_accessed=1 << 22, transcendentals=0),
        name="far",
    )(n_far, n_farpair, *shared, *early_own, *early_pair)
    got1 = swap(send0, 2)
    cut = prow * 3 // 4
    halves = (shape((cut, width)), shape((prow - cut, width)))
    part1, send1a, send1b = call(
        functools.partial(late_kernel, hdim), (part_shape,) + halves, 8 * MIB, 6 * mul
    )(n_far, *shared, *kv_own, *kv_pair, k_far, v_far)
    got0a = swap(send1a, 2)
    got0b = swap(send1b, 2)
    late_rows = call(copy_kernel, shape(rows.shape, rows.dtype), MIB, 1000)(rows)

    def merge(keep, start, x, part, got, late_rows, *after):
        count = got.shape[0]
        outs = (shape((count, width)),) * keep + (shape((count // 4, 4 * width)),)
        return pl.pallas_call(
            functools.partial(merge_kernel, keep, start),
            out_shape=outs,
            in_specs=[VMEM] * 4 + [ANY] * len(after),
            scratch_shapes=[pltpu.VMEM((width // 128, count, 128), jnp.float32)],
            compiler_params=pltpu.CompilerParams(vmem_limit_bytes=4 * MIB),
            cost_estimate=pl.CostEstimate(flops=mul // 4, bytes_accessed=1 << 20, transcendentals=0),
        )(x, part, got, late_rows, *after)

    fc1 = pltpu.with_memory_space_constraint(fc1_weight, pltpu.VMEM)
    (blocks1,) = merge(0, 0, x_far, part1, got1, late_rows)
    pair1 = swap(blocks1, 1)
    flops = prow * 4 * width * hidden
    early = call(hidden_kernel, shape((prow // 2, hidden)), 4 * MIB, flops)(blocks1, pair1, fc1, rows)
    vit_a, blocks_a = merge(1, 0, x_own, part0, got0a, late_rows, early)
    pair_a = swap(blocks_a, 1)
    late_rows = call(copy_kernel, shape(rows.shape, rows.dtype), MIB, 1000)(late_rows)
    vit_b, blocks_b = merge(1, cut, x_own, part0, got0b, late_rows)
    pair_b = swap(blocks_b, 1)
    parts = hidden // 256
    merged, vit_out = pl.pallas_call(
        last_kernel,
        out_shape=(shape((prow, hidden)), shape((prow, width))),
        out_specs=[HBM] * 2,
        scratch_shapes=[
            pltpu.VMEM((parts, prow // 2, 256), jnp.bfloat16),
            pltpu.SemaphoreType.DMA((3 + 2 * parts,)),
        ],
        compiler_params=pltpu.CompilerParams(vmem_limit_bytes=4 * MIB),
        cost_estimate=pl.CostEstimate(flops=flops, bytes_accessed=1 << 24, transcendentals=0),
        name="hidden0",
    )(blocks_a, blocks_b, pair_a, pair_b, fc1, rows, vit_a, vit_b, early)
    return vit_out, merged


def rotate(values, positions, nheads):
    count = values.shape[0]
    hdim = values.shape[1] // nheads
    quarter = hdim // 4
    inv = 1.0 / 10000.0 ** (jnp.arange(quarter, dtype=jnp.float32) * 2.0 / (hdim // 2))
    rows = positions[0].astype(jnp.float32)[:, None] * inv
    cols = positions[1].astype(jnp.float32)[:, None] * inv
    angle = jnp.concatenate([rows, cols, rows, cols], axis=1)
    cosine = jnp.cos(angle)[:, None, :]
    sine = jnp.sin(angle)[:, None, :]
    shaped = values.reshape(count, nheads, hdim)
    half = hdim // 2
    turned = jnp.concatenate([-shaped[..., half:], shaped[..., :half]], axis=-1)
    return (shaped * cosine + turned * sine).reshape(count, nheads * hdim)


def attend_blocks(query, keys, value, nheads, hdim):
    count = query.shape[0]
    block = min(512, count)
    qblocks = query.reshape(count // block, block, nheads, hdim)
    kshaped = keys.reshape(count, nheads, hdim)
    vshaped = value.reshape(count, nheads, hdim)
    scale = 1.0 / jnp.sqrt(jnp.float32(hdim))

    def one_block(qpart):
        scores = jnp.einsum("bhd,khd->hbk", qpart, kshaped, preferred_element_type=jnp.float32) * scale
        top = jnp.max(scores, axis=-1, keepdims=True)
        expo = jnp.exp(scores - top)
        weights = (expo / jnp.sum(expo, axis=-1, keepdims=True)).astype(jnp.bfloat16)
        result = jnp.einsum("hbk,khd->bhd", weights, vshaped, preferred_element_type=jnp.float32)
        return result.astype(jnp.bfloat16).reshape(block, nheads * hdim)

    return lax.map(one_block, qblocks).reshape(count, nheads * hdim)


def any_size(
    patches,
    pos_ids,
    norm_gain,
    norm_bias,
    qkv_weight,
    qkv_bias,
    proj_weight,
    proj_bias,
    merge_gain,
    merge_bias,
    fc1_weight,
    fc1_bias,
):
    groups = lax.axis_size("sp")
    where = lax.axis_index("sp")
    prow, width = patches.shape
    heads_local = HEADS // groups
    hdim = width // HEADS
    local_width = width // groups
    xfloat = patches.astype(jnp.float32)
    normed = layer_norm(xfloat, norm_gain, norm_bias).astype(jnp.bfloat16)
    bias_local = lax.dynamic_slice_in_dim(qkv_bias, where * local_width, local_width, 1)
    qkv = (
        jnp.einsum(
            "pd,dcn->pcn",
            lax.all_gather(normed, "sp", axis=0, tiled=True),
            qkv_weight,
            preferred_element_type=jnp.float32,
        )
        + bias_local[None]
    )
    query = rotate(qkv[:, 0], pos_ids, heads_local).astype(jnp.bfloat16)
    keys = rotate(qkv[:, 1], pos_ids, heads_local).astype(jnp.bfloat16)
    value = qkv[:, 2].astype(jnp.bfloat16)
    attended = attend_blocks(query, keys, value, heads_local, hdim)
    returned = lax.all_to_all(attended, "sp", split_axis=0, concat_axis=1, tiled=True)
    projected = jnp.dot(
        returned,
        lax.all_gather(proj_weight, "sp", axis=0, tiled=True),
        preferred_element_type=jnp.float32,
    )
    vit_out = (xfloat + projected + proj_bias).astype(jnp.bfloat16)
    zn = layer_norm(vit_out.astype(jnp.float32), merge_gain, merge_bias).astype(jnp.bfloat16)
    blocks = zn.reshape(prow // 4, 4 * width)
    hidden = (
        jnp.dot(
            lax.all_gather(blocks, "sp", axis=0, tiled=True),
            fc1_weight,
            preferred_element_type=jnp.float32,
        )
        + fc1_bias
    )
    merged_hidden = jax.nn.gelu(hidden, approximate=False).astype(jnp.bfloat16)
    return (vit_out, merged_hidden)


def per_device(*args):
    if lax.axis_size("sp") == 4:
        return two_chips(*args)
    return any_size(*args)


def solution(mesh):
    return jax.shard_map(
        per_device,
        mesh=mesh,
        in_specs=(
            P(("img", "sp"), None),
            P(None, "img"),
            P(),
            P(),
            P(None, None, "sp"),
            P(),
            P("sp", None),
            P(),
            P(),
            P(),
            P(None, "sp"),
            P("sp"),
        ),
        out_specs=(P(("img", "sp"), None), P("img", "sp")),
        check_vma=False,
    )
```

```python
import functools
import math

import jax
import jax.numpy as jnp
from jax import lax
from jax.experimental import pallas as pl
from jax.experimental.pallas import tpu as pltpu
from jax.sharding import PartitionSpec as P


HEADS = 16
EPS = 1e-06
MIB = 1 << 20
VMEM = pl.BlockSpec(memory_space=pltpu.VMEM)
ANY = pl.BlockSpec(memory_space=pl.ANY)
HBM = pl.BlockSpec(memory_space=pltpu.HBM)
NT = (((1,), (1,)), ((), ()))
TN = (((0,), (0,)), ((), ()))
NN = (((1,), (0,)), ((), ()))


def layer_norm(values, gain, bias):
    mean = jnp.mean(values, axis=-1, keepdims=True)
    centered = values - mean
    var = jnp.mean(centered * centered, axis=-1, keepdims=True)
    return centered * lax.rsqrt(var + EPS) * gain + bias


def dot(a, b, dims):
    return lax.dot_general(a, b, dims, preferred_element_type=jnp.float32)


def call(kernel, outs, nbytes, flops):
    return pl.pallas_call(
        kernel,
        out_shape=outs,
        compiler_params=pltpu.CompilerParams(vmem_limit_bytes=nbytes),
        cost_estimate=pl.CostEstimate(flops=flops, bytes_accessed=1 << 20, transcendentals=0),
    )


def setup_kernel(hdim, count, *refs):
    sources, rest = refs[:count], refs[count:]
    x, wown, pall, normed, rows, qcol, cosine, sine, pos, qkv_bias = rest[:10]
    vectors, sems = rest[10:-1], rest[-1]
    targets = (x, pos, qkv_bias) + tuple(vectors) + (pall.at[pl.ds(0, pall.shape[0] // 2)], wown)
    copies = [pltpu.make_async_copy(a, b, sems.at[n]) for n, (a, b) in enumerate(zip(sources, targets))]
    for copy in copies:
        copy.start()
    prow, width = x.shape
    me = lax.axis_index("sp")
    quarter = hdim // 4
    feature = lax.broadcasted_iota(jnp.int32, (2 * quarter, prow), 0)
    second = feature >= quarter
    power = jnp.where(second, feature - quarter, feature).astype(jnp.float32)
    inv = jnp.exp(power * (-2.0 * math.log(10000.0) / (hdim // 2)))
    rows[...] = jnp.zeros_like(rows)
    for copy in copies[:-2]:
        copy.wait()
    for k in range(4):
        at = pl.ds(pl.multiple_of((me ^ k) * prow, prow), prow)
        place = jnp.where(second, pos[1:2, at], pos[0:1, at]).astype(jnp.float32)
        angle = place * inv
        cosine[:, k * prow : (k + 1) * prow] = jnp.cos(angle)
        sine[:, k * prow : (k + 1) * prow] = jnp.sin(angle)
    for at, vector in enumerate(vectors):
        rows[at : at + 1, :] = vector[...].reshape(1, width)
    cube = jnp.concatenate([qkv_bias[...], jnp.zeros((5, width), jnp.float32)], axis=0)
    qcol[...] = cube.T
    value = layer_norm(x[...].astype(jnp.float32), rows[0:1, :], rows[1:2, :])
    normed[...] = value.astype(jnp.bfloat16)
    for copy in copies[-2:]:
        copy.wait()


def copy_kernel(x, out):
    out[...] = x[...]


def norm_kernel(start, x, rows, *rest):
    out = rest[-1]
    value = x[start : start + out.shape[0], :].astype(jnp.float32)
    out[...] = layer_norm(value, rows[0:1, :], rows[1:2, :]).astype(jnp.bfloat16)


def column(qcol, owner, local, c):
    return qcol[pl.ds(pl.multiple_of(owner * local, 8), local), c : c + 1]


def rotated(raw, cos, sin, hdim):
    half = hdim // 2
    pieces = []
    for at in range(0, raw.shape[0], hdim):
        top, low = raw[at : at + half], raw[at + half : at + hdim]
        pieces += [top * cos - low * sin, low * cos + top * sin]
    return jnp.concatenate(pieces, axis=0).astype(jnp.bfloat16)


def paired(query, hdim):
    zero = jnp.zeros((hdim, query.shape[1]), query.dtype)
    rows = []
    for at in range(0, query.shape[0], 2 * hdim):
        rows.append(jnp.concatenate([query[at : at + hdim], zero], axis=1))
        rows.append(jnp.concatenate([zero, query[at + hdim : at + 2 * hdim]], axis=1))
    return jnp.concatenate(rows, axis=0)


def near_kernel(hdim, side, xa, xb, weight, qcol, cosine, sine, *rest):
    qout, kout, vout, tops, sums, outs = rest
    scale = math.log2(math.e) / math.sqrt(hdim)
    local = weight.shape[0] // 3
    rows = xa.shape[0]
    owner = lax.axis_index("sp") ^ side
    normed = jnp.concatenate([xa[...], xb[...]], axis=0)
    cos, sin = cosine[:, : 2 * rows], sine[:, : 2 * rows]
    query = dot(weight[0:local, :], normed[:rows], NT) + column(qcol, owner, local, 0)
    query = paired(rotated(query, cos[:, :rows], sin[:, :rows], hdim), hdim)
    keyval = dot(weight[local:, :], normed, NT)
    key = rotated(keyval[:local] + column(qcol, owner, local, 1), cos, sin, hdim)
    value = (keyval[local:] + column(qcol, owner, local, 2)).astype(jnp.bfloat16)
    qout[...] = query
    kout[...] = key
    vout[...] = value
    for p in range(local // (2 * hdim)):
        f = slice(2 * p * hdim, 2 * (p + 1) * hdim)
        scores = dot(key[f], query[f], TN)
        top = jnp.max(scores, axis=0, keepdims=True)
        expo = jnp.exp2((scores - top) * scale)
        tops[p : p + 1, :] = top
        sums[p : p + 1, :] = jnp.sum(expo, axis=0, keepdims=True)
        total = dot(value[f], expo.astype(jnp.bfloat16), NN)
        outs[f.start : f.start + hdim, :] = total[:hdim, :rows]
        outs[f.start + hdim : f.stop, :] = total[hdim:, rows:]


def gather_kernel(ppair, half, after, pall, sem):
    del half, after
    count = ppair.shape[0]
    copy = pltpu.make_async_copy(ppair, pall.at[pl.ds(count, count)], sem)
    copy.start()
    copy.wait()


def far_kernel(hdim, xa, xb, wown, wpair, pall, qcol, cosine, sine, *refs):
    scale = math.log2(math.e) / math.sqrt(hdim)
    near, (part, send, kout, vout, raw, expos, attended) = (refs[:4], refs[4:8]), refs[8:]
    local = wown.shape[0] // 3
    rows = xa.shape[0]
    me = lax.axis_index("sp")
    normed = jnp.concatenate([xa[...], xb[...]], axis=0)
    cos, sin = cosine[:, 2 * rows :], sine[:, 2 * rows :]
    pairs = local // (2 * hdim)
    tops, shrinks, invs = {}, {}, {}

    def place(side, p):
        f = slice(2 * p * hdim, 2 * (p + 1) * hdim)
        return f, slice(side * local + f.start, side * local + f.stop)

    def project(side, c):
        weight = (wown, wpair)[side][c * local : (c + 1) * local, :]
        return dot(weight, normed, NT) + column(qcol, me ^ side, local, c)

    for side in range(2):
        kout[side * local : (side + 1) * local, :] = rotated(project(side, 1), cos, sin, hdim)
    for side in range(2):
        vout[side * local : (side + 1) * local, :] = project(side, 2).astype(jnp.bfloat16)
    for side in range(2):
        for p in range(pairs):
            f, g = place(side, p)
            scores = dot(kout[g, :], near[side][0][f, :], TN)
            raw[side * pairs + p] = scores
            old = near[side][1][p : p + 1, :]
            tops[side, p] = jnp.maximum(old, jnp.max(scores, axis=0, keepdims=True))
    for side in range(2):
        for p in range(pairs):
            top = tops[side, p]
            expo = jnp.exp2((raw[side * pairs + p] - top) * scale)
            expos[side * pairs + p] = expo.astype(jnp.bfloat16)
            shrink = jnp.exp2((near[side][1][p : p + 1, :] - top) * scale)
            shrinks[side, p] = shrink
            sums = near[side][2][p : p + 1, :]
            invs[side, p] = 1.0 / (sums * shrink + jnp.sum(expo, axis=0, keepdims=True))
    for side in range(2):
        for p in range(pairs):
            f, g = place(side, p)
            late = dot(vout[g, :], expos[side * pairs + p], NN)
            for h in range(2):
                lanes = slice(h * rows, (h + 1) * rows)
                feats = slice(h * hdim, (h + 1) * hdim)
                early = near[side][3][f.start + h * hdim : f.start + (h + 1) * hdim, :]
                mixed = (early * shrinks[side, p][:, lanes] + late[feats, lanes]) * invs[side, p][:, lanes]
                attended[g.start + h * hdim : g.start + (h + 1) * hdim, :] = mixed.astype(jnp.bfloat16)
    total = dot(attended[...], pall[...], TN)
    part[...] = total
    send[...] = total.astype(jnp.bfloat16)


def late_kernel(hdim, x, wown, wpair, pall, qcol, cosine, sine, kna, vna, knb, vnb, kf, vf, part, send0, send1):
    scale = math.log2(math.e) / math.sqrt(hdim)
    local = wown.shape[0] // 3
    rows = x.shape[0]
    me = lax.axis_index("sp")
    pieces = []
    for side, weight in enumerate((wown, wpair)):
        query = dot(weight[:local, :], x[...], NT) + column(qcol, me ^ side, local, 0)
        far = slice(3 * rows, 4 * rows)
        query = paired(rotated(query, cosine[:, far], sine[:, far], hdim), hdim)
        for at in range(0, local, 2 * hdim):
            f = slice(side * local + at, side * local + at + 2 * hdim)
            g = slice(at, at + 2 * hdim)
            kn, vn = ((kna, vna), (knb, vnb))[side]
            both = query[g]
            sn = dot(kn[g, :], both, TN)
            sf = dot(kf[f, :], both, TN)
            top = jnp.maximum(jnp.max(sn, axis=0, keepdims=True), jnp.max(sf, axis=0, keepdims=True))
            en = jnp.exp2((sn - top) * scale)
            ef = jnp.exp2((sf - top) * scale)
            inv = 1.0 / (jnp.sum(en, axis=0, keepdims=True) + jnp.sum(ef, axis=0, keepdims=True))
            mixed = dot(vn[g, :], (en * inv).astype(jnp.bfloat16), NN)
            mixed = (mixed + dot(vf[f, :], (ef * inv).astype(jnp.bfloat16), NN)).astype(jnp.bfloat16)
            pieces += [mixed[:hdim, :rows], mixed[hdim:, rows:]]
    total = dot(jnp.concatenate(pieces, axis=0), pall[...], TN)
    part[...] = total
    cut = send0.shape[0]
    send0[...] = total[:cut].astype(jnp.bfloat16)
    send1[...] = total[cut:].astype(jnp.bfloat16)


def merge_kernel(keep, start, x, part, got, rows, *rest):
    blocks, scratch = rest[-2], rest[-1]
    width = x.shape[1]
    place = slice(start, start + got.shape[0])
    value = x[place, :].astype(jnp.float32) + (part[place, :] + got[...].astype(jnp.float32)) + rows[2:3, :]
    rounded = value.astype(jnp.bfloat16)
    if keep:
        rest[-3][...] = rounded
    normed = layer_norm(rounded.astype(jnp.float32), rows[3:4, :], rows[4:5, :])
    count = got.shape[0] // 4
    lanes = scratch.shape[2]
    for t in range(width // lanes):
        scratch[t] = normed[:, t * lanes : (t + 1) * lanes]
        for j in range(4):
            at = j * width + t * lanes
            blocks[:, at : at + lanes] = scratch[t, pl.ds(j, count, stride=4), :].astype(jnp.bfloat16)


def gelu(v):
    return 0.5 * v * (1.0 + lax.erf(v * math.sqrt(0.5)))


def hidden_kernel(own, pair, weight, rows, out):
    core = lax.axis_index("sp") % 2
    count = own.shape[0]
    both = jnp.concatenate([own[...], pair[...]] * 2, axis=0)
    hid = gelu(dot(both, weight[...], NN)[: 2 * count] + rows[5:6, :]).astype(jnp.bfloat16)
    for half, place in enumerate((1 - core, core)):
        out[pl.ds(pl.multiple_of(place * count, count), count), :] = hid[half * count : (half + 1) * count]


def last_kernel(own0, own1, pair0, pair1, weight, rows, vit0, vit1, early, out, vout, stage, sems):
    me = lax.axis_index("sp")
    chip, core = me // 2, me % 2
    count = own0.shape[0] + own1.shape[0]
    cut, rest = vit0.shape[0], vit1.shape[0]
    at = lambda start: pl.ds(pl.multiple_of(start, count), count)
    there = out.at[pl.ds(pl.multiple_of((1 - chip) * 2 * count, count), 2 * count)]
    copies = [
        pltpu.make_async_copy(vit0, vout.at[pl.ds(0, cut)], sems.at[0]),
        pltpu.make_async_copy(vit1, vout.at[pl.ds(cut, rest)], sems.at[1]),
        pltpu.make_async_copy(early, there, sems.at[2]),
    ]
    for copy in copies:
        copy.start()
    both = jnp.concatenate([x[...] for x in (own0, own1, pair0, pair1)] * 2, axis=0)
    step = stage.shape[2]
    for n in range(stage.shape[0]):
        cols = slice(n * step, (n + 1) * step)
        value = dot(both, weight[:, cols], NN)[: 2 * count] + rows[5:6, cols]
        stage[n] = gelu(value).astype(jnp.bfloat16)
        for side, place in enumerate((core, 1 - core)):
            copy = pltpu.make_async_copy(
                stage.at[n, pl.ds(side * count, count)],
                out.at[at(chip * 2 * count + place * count), pl.ds(n * step, step)],
                sems.at[3 + 2 * n + side],
            )
            copy.start()
            copies.append(copy)
    for copy in copies:
        copy.wait()


def shape(dims, dtype=jnp.bfloat16):
    return jax.ShapeDtypeStruct(dims, dtype)


def two_chips(
    patches,
    pos_ids,
    norm_gain,
    norm_bias,
    qkv_weight,
    qkv_bias,
    proj_weight,
    proj_bias,
    merge_gain,
    merge_bias,
    fc1_weight,
    fc1_bias,
):
    prow, width = patches.shape
    hdim = width // HEADS
    local = qkv_weight.shape[2]
    hidden = fc1_weight.shape[1]

    def swap(value, bit):
        return lax.ppermute(value, "sp", [(i, i ^ bit) for i in range(4)])

    weight = qkv_weight.transpose(1, 2, 0).reshape(3 * local, width)
    x_far = swap(patches, 2)
    x_pair = swap(patches, 1)
    w_pair = swap(weight, 1)
    p_pair = swap(proj_weight, 1)

    both = 2 * local
    mul = 2 * prow * width * local * 2
    table = shape((hdim // 2, 4 * prow), jnp.float32)

    sources = (patches, pos_ids, qkv_bias, norm_gain, norm_bias, proj_bias, merge_gain, merge_bias, fc1_bias)
    sources += (proj_weight, weight)
    held = lambda v: pltpu.VMEM(v.shape, v.dtype)
    x_own, w_own, p_half, n_own, rows, qcol, cos, sin = pl.pallas_call(
        functools.partial(setup_kernel, hdim, len(sources)),
        out_shape=(
            held(patches),
            held(weight),
            pltpu.VMEM((both, width), proj_weight.dtype),
            shape((prow, width)),
            shape((8, width), jnp.float32),
            shape((width, 8), jnp.float32),
            table,
            table,
        ),
        in_specs=[HBM] * len(sources),
        scratch_shapes=[held(v) for v in sources[1:-2]] + [pltpu.SemaphoreType.DMA((len(sources),))],
        compiler_params=pltpu.CompilerParams(vmem_limit_bytes=4 * MIB),
        cost_estimate=pl.CostEstimate(flops=mul, bytes_accessed=1 << 22, transcendentals=0),
        name="setup",
    )(*(pltpu.with_memory_space_constraint(v, pltpu.HBM) for v in sources))

    def norm(x, start, count, *after):
        return pl.pallas_call(
            functools.partial(norm_kernel, start),
            out_shape=shape((count, width)),
            in_specs=[VMEM] * 2 + [ANY] * len(after),
            compiler_params=pltpu.CompilerParams(vmem_limit_bytes=4 * MIB),
            cost_estimate=pl.CostEstimate(flops=mul // 4, bytes_accessed=1 << 20, transcendentals=0),
        )(x, rows, *after)

    n_pair = norm(x_pair, 0, prow)
    flat = shape((local, 2 * prow))
    state = shape((local // (2 * hdim), 2 * prow), jnp.float32)
    near_shape = (flat, flat, flat, state, state, shape((local, prow), jnp.float32))

    def near(side, weight):
        return call(
            functools.partial(near_kernel, hdim, side), near_shape, 8 * MIB, 4 * mul
        )(n_own, n_pair, weight, qcol, cos, sin)

    q, *kv_own, tops, sums, outs = near(0, w_own)
    early_own = (q, tops, sums, outs)
    q, *kv_pair, tops, sums, outs = near(1, w_pair)
    early_pair = (q, tops, sums, outs)

    n_far = norm(x_far, 0, prow, early_own[1], early_pair[1])
    n_farpair = swap(n_far, 1)
    x_cross = swap(x_far, 1)
    p_all = pl.pallas_call(
        gather_kernel,
        out_shape=pltpu.VMEM((both, width), proj_weight.dtype),
        in_specs=[VMEM, VMEM, ANY],
        input_output_aliases={1: 0},
        scratch_shapes=[pltpu.SemaphoreType.DMA],
        compiler_params=pltpu.CompilerParams(vmem_limit_bytes=2 * MIB),
        cost_estimate=pl.CostEstimate(flops=mul // 4, bytes_accessed=1 << 20, transcendentals=0),
        name="gather_proj",
    )(p_pair, p_half, n_far)
    tall = shape((both, 2 * prow))
    shared = (w_own, w_pair, p_all, qcol, cos, sin)
    part_shape = shape((prow, width), jnp.float32)
    folds = both // (2 * hdim)
    part0, send0, k_far, v_far = pl.pallas_call(
        functools.partial(far_kernel, hdim),
        out_shape=(part_shape, shape((prow, width)), tall, tall),
        scratch_shapes=[
            pltpu.VMEM((folds, 2 * prow, 2 * prow), jnp.float32),
            pltpu.VMEM((folds, 2 * prow, 2 * prow), jnp.bfloat16),
            pltpu.VMEM((both, prow), jnp.bfloat16),
        ],
        compiler_params=pltpu.CompilerParams(vmem_limit_bytes=8 * MIB),
        cost_estimate=pl.CostEstimate(flops=6 * mul, bytes_accessed=1 << 22, transcendentals=0),
        name="far",
    )(n_far, n_farpair, *shared, *early_own, *early_pair)
    got1 = swap(send0, 3)
    cut = prow * 3 // 4
    halves = (shape((cut, width)), shape((prow - cut, width)))
    part1, send1a, send1b = call(
        functools.partial(late_kernel, hdim), (part_shape,) + halves, 8 * MIB, 6 * mul
    )(n_farpair, *shared, *kv_own, *kv_pair, k_far, v_far)
    got0a = swap(send1a, 3)
    got0b = swap(send1b, 3)
    late_rows = call(copy_kernel, shape(rows.shape, rows.dtype), MIB, 1000)(rows)

    def merge(keep, start, x, part, got, late_rows, *after):
        count = got.shape[0]
        outs = (shape((count, width)),) * keep + (shape((count // 4, 4 * width)),)
        return pl.pallas_call(
            functools.partial(merge_kernel, keep, start),
            out_shape=outs,
            in_specs=[VMEM] * 4 + [ANY] * len(after),
            scratch_shapes=[pltpu.VMEM((width // 128, count, 128), jnp.float32)],
            compiler_params=pltpu.CompilerParams(vmem_limit_bytes=4 * MIB),
            cost_estimate=pl.CostEstimate(flops=mul // 4, bytes_accessed=1 << 20, transcendentals=0),
        )(x, part, got, late_rows, *after)

    fc1 = pltpu.with_memory_space_constraint(fc1_weight, pltpu.VMEM)
    (blocks1,) = merge(0, 0, x_cross, part1, got1, late_rows)
    pair1 = swap(blocks1, 1)
    flops = prow * 4 * width * hidden
    early = call(hidden_kernel, shape((prow // 2, hidden)), 4 * MIB, flops)(blocks1, pair1, fc1, rows)
    vit_a, blocks_a = merge(1, 0, x_own, part0, got0a, late_rows, early)
    pair_a = swap(blocks_a, 1)
    late_rows = call(copy_kernel, shape(rows.shape, rows.dtype), MIB, 1000)(late_rows)
    vit_b, blocks_b = merge(1, cut, x_own, part0, got0b, late_rows)
    pair_b = swap(blocks_b, 1)
    parts = hidden // 256
    merged, vit_out = pl.pallas_call(
        last_kernel,
        out_shape=(shape((prow, hidden)), shape((prow, width))),
        out_specs=[HBM] * 2,
        scratch_shapes=[
            pltpu.VMEM((parts, prow // 2, 256), jnp.bfloat16),
            pltpu.SemaphoreType.DMA((3 + 2 * parts,)),
        ],
        compiler_params=pltpu.CompilerParams(vmem_limit_bytes=4 * MIB),
        cost_estimate=pl.CostEstimate(flops=flops, bytes_accessed=1 << 24, transcendentals=0),
        name="hidden0",
    )(blocks_a, blocks_b, pair_a, pair_b, fc1, rows, vit_a, vit_b, early)
    return vit_out, merged


def rotate(values, positions, nheads):
    count = values.shape[0]
    hdim = values.shape[1] // nheads
    quarter = hdim // 4
    inv = 1.0 / 10000.0 ** (jnp.arange(quarter, dtype=jnp.float32) * 2.0 / (hdim // 2))
    rows = positions[0].astype(jnp.float32)[:, None] * inv
    cols = positions[1].astype(jnp.float32)[:, None] * inv
    angle = jnp.concatenate([rows, cols, rows, cols], axis=1)
    cosine = jnp.cos(angle)[:, None, :]
    sine = jnp.sin(angle)[:, None, :]
    shaped = values.reshape(count, nheads, hdim)
    half = hdim // 2
    turned = jnp.concatenate([-shaped[..., half:], shaped[..., :half]], axis=-1)
    return (shaped * cosine + turned * sine).reshape(count, nheads * hdim)


def attend_blocks(query, keys, value, nheads, hdim):
    count = query.shape[0]
    block = min(512, count)
    qblocks = query.reshape(count // block, block, nheads, hdim)
    kshaped = keys.reshape(count, nheads, hdim)
    vshaped = value.reshape(count, nheads, hdim)
    scale = 1.0 / jnp.sqrt(jnp.float32(hdim))

    def one_block(qpart):
        scores = jnp.einsum("bhd,khd->hbk", qpart, kshaped, preferred_element_type=jnp.float32) * scale
        top = jnp.max(scores, axis=-1, keepdims=True)
        expo = jnp.exp(scores - top)
        weights = (expo / jnp.sum(expo, axis=-1, keepdims=True)).astype(jnp.bfloat16)
        result = jnp.einsum("hbk,khd->bhd", weights, vshaped, preferred_element_type=jnp.float32)
        return result.astype(jnp.bfloat16).reshape(block, nheads * hdim)

    return lax.map(one_block, qblocks).reshape(count, nheads * hdim)


def any_size(
    patches,
    pos_ids,
    norm_gain,
    norm_bias,
    qkv_weight,
    qkv_bias,
    proj_weight,
    proj_bias,
    merge_gain,
    merge_bias,
    fc1_weight,
    fc1_bias,
):
    groups = lax.axis_size("sp")
    where = lax.axis_index("sp")
    prow, width = patches.shape
    heads_local = HEADS // groups
    hdim = width // HEADS
    local_width = width // groups
    xfloat = patches.astype(jnp.float32)
    normed = layer_norm(xfloat, norm_gain, norm_bias).astype(jnp.bfloat16)
    bias_local = lax.dynamic_slice_in_dim(qkv_bias, where * local_width, local_width, 1)
    qkv = (
        jnp.einsum(
            "pd,dcn->pcn",
            lax.all_gather(normed, "sp", axis=0, tiled=True),
            qkv_weight,
            preferred_element_type=jnp.float32,
        )
        + bias_local[None]
    )
    query = rotate(qkv[:, 0], pos_ids, heads_local).astype(jnp.bfloat16)
    keys = rotate(qkv[:, 1], pos_ids, heads_local).astype(jnp.bfloat16)
    value = qkv[:, 2].astype(jnp.bfloat16)
    attended = attend_blocks(query, keys, value, heads_local, hdim)
    returned = lax.all_to_all(attended, "sp", split_axis=0, concat_axis=1, tiled=True)
    projected = jnp.dot(
        returned,
        lax.all_gather(proj_weight, "sp", axis=0, tiled=True),
        preferred_element_type=jnp.float32,
    )
    vit_out = (xfloat + projected + proj_bias).astype(jnp.bfloat16)
    zn = layer_norm(vit_out.astype(jnp.float32), merge_gain, merge_bias).astype(jnp.bfloat16)
    blocks = zn.reshape(prow // 4, 4 * width)
    hidden = (
        jnp.dot(
            lax.all_gather(blocks, "sp", axis=0, tiled=True),
            fc1_weight,
            preferred_element_type=jnp.float32,
        )
        + fc1_bias
    )
    merged_hidden = jax.nn.gelu(hidden, approximate=False).astype(jnp.bfloat16)
    return (vit_out, merged_hidden)


def per_device(*args):
    if lax.axis_size("sp") == 4:
        return two_chips(*args)
    return any_size(*args)


def solution(mesh):
    return jax.shard_map(
        per_device,
        mesh=mesh,
        in_specs=(
            P(("img", "sp"), None),
            P(None, "img"),
            P(),
            P(),
            P(None, None, "sp"),
            P(),
            P("sp", None),
            P(),
            P(),
            P(),
            P(None, "sp"),
            P("sp"),
        ),
        out_specs=(P(("img", "sp"), None), P("img", "sp")),
        check_vma=False,
    )
```
